32 devices in a mesh: seq: 4 (over y, x), tp: 4 (over z), grp: 2 (over core).
Axes of the slice: x: 2, y: 2, z: 4, core: 2. Of those that a mesh axis runs over, the one named last changes fastest.
Arguments:
- queries: bfloat16 [4, 64, 128], P('grp', 'tp'), may hold values from -2000 to 2000
- cache_pool: bfloat16 [512, 8, 2, 128, 128], P(('seq', 'grp'), 'tp'), may hold values from -6 to 6
- block_scale: bfloat16 [512, 8, 2], P(('seq', 'grp'), 'tp'), may hold values from 0.29 to 3
- block_table: int32 [4, 128], replicated, may hold values from 0 to 511, as said below
- lengths: int32 [4], replicated, may hold values from 128 to 16384
- output_weight: bfloat16 [8192, 8192], P('tp', ('seq', 'grp')), may hold values from -0.0625 to 0.0625
Outputs:
- attention_output: bfloat16 [4, 8192], P('tp', ('seq', 'grp'))
- decode_cache: bfloat16 [4, 128, 8, 2, 128, 128], P('grp', 'seq', 'tp')
- decode_scale: bfloat16 [4, 128, 8, 2], P('grp', 'seq', 'tp')
The draws below stay inside these ranges and needn't reach their ends.
Inputs may be any that keep to these rules, and one draw needn't show every extreme that they name: block_table names every pool slot exactly once. Take any run of 64 slots starting at a multiple of 64, any group of 2 consecutive requests starting at a multiple of 2, and any range of 32 block positions starting at a multiple of 32: exactly 8 slots of the run hold blocks of those requests at those positions.
All inputs are finite; a program needn't handle non-finite values.
Results may differ from the reference program's by a relative error of at most 0.014.
Values may be sent and summed in bfloat16 or wider, within the bound.
A program may use at most 64 MiB of HBM per device.

```python
import math
import jax
import jax.numpy as jnp
from jax import lax

D = 8192
H = 64
KVH = 8
HD = 128
BLK = 128
NB = 128
BPG = 2
BATCH = 4
POOL = 512
POOL_DEV = 64
NBQ = 32
CAP = 8
N_SEQ = 4
N_GRP = 2


def block_layout(key):
    base_key = jax.random.fold_in(key, 7)
    pair_keys = jax.random.split(jax.random.fold_in(base_key, 1), N_GRP * N_SEQ)
    spread = jax.vmap(lambda sub_key: jax.random.permutation(sub_key, BPG * NBQ))(pair_keys).astype(jnp.int32)
    owner_keys = jax.random.split(jax.random.fold_in(base_key, 2), N_SEQ * N_GRP)
    places = jax.vmap(lambda sub_key: jax.random.permutation(sub_key, POOL_DEV))(owner_keys).astype(jnp.int32)
    owners = spread // CAP
    within = spread % CAP
    pair_ids = jnp.arange(N_GRP * N_SEQ, dtype=jnp.int32)[:, None]
    column = pair_ids * CAP + within
    slot_ids = owners * POOL_DEV + places[owners, column]
    return slot_ids.reshape(N_GRP, N_SEQ, BPG, NBQ).transpose(0, 2, 1, 3).reshape(BATCH, NB).astype(jnp.int32)


def cache_law(key):
    base_key = jax.random.fold_in(key, 13)
    pool_shape = (POOL, KVH, 2, BLK, HD)
    pool_data = jnp.clip(jax.random.normal(jax.random.fold_in(base_key, 1), pool_shape, jnp.float32), -6.0, 6.0)
    scale_data = jnp.exp(jax.random.uniform(jax.random.fold_in(base_key, 2), (POOL, KVH, 2), jnp.float32, math.log(0.5), math.log(2.0)))
    query_data = jnp.clip(2.5 * jax.random.normal(jax.random.fold_in(base_key, 3), (BATCH, H, HD), jnp.float32), -15.0, 15.0)
    return (pool_data, scale_data, query_data)


def draw_queries(key, part):
    return cache_law(key)[2].astype(jnp.bfloat16)


def draw_cache_pool(key, part):
    return cache_law(key)[0].astype(jnp.bfloat16)


def draw_block_scale(key, part):
    return cache_law(key)[1].astype(jnp.bfloat16)


def draw_block_table(key, part):
    return block_layout(key)


def set_ends(drawn, rng, smallest, high):
    spot = [jax.random.randint(jax.random.fold_in(rng, axis), (), 0, length) for axis, length in enumerate(drawn.shape)]
    widest = drawn.shape.index(max(drawn.shape))
    beside = spot[:widest] + [(spot[widest] + 1) % drawn.shape[widest]] + spot[widest + 1:]
    return drawn.at[tuple(spot)].set(smallest).at[tuple(beside)].set(high)


def level_of(own_key, shape, cuts, least, largest):
    def one(position, blocks):
        steps = jax.random.uniform(jax.random.fold_in(jax.random.fold_in(own_key, 6), position), (blocks,), jnp.float32, least / len(cuts), largest / len(cuts))
        return jnp.repeat(jnp.exp(steps), shape[position] // blocks).reshape((-1,) + (1,) * (len(shape) - position - 1))

    factor_of = one(*cuts[0])
    for cut in cuts[1:]:
        factor_of = factor_of * one(*cut)
    return factor_of


def gaussian(rng, extent, deviation, most, cuts=(), held_as=jnp.bfloat16):
    array = deviation * jax.random.normal(rng, extent, jnp.float32)
    if cuts:
        array = array * level_of(rng, extent, cuts, -0.22, 0.18)
    return jnp.clip(array, -most, most).astype(held_as)


def setup_inputs(seed: int = 0) -> dict:
    key_list = jax.random.split(jax.random.key(seed), 7)
    return {
        "queries": draw_queries(jax.random.fold_in(key_list[6], 71), 0),
        "cache_pool": draw_cache_pool(jax.random.fold_in(key_list[6], 71), 0),
        "block_scale": draw_block_scale(jax.random.fold_in(key_list[6], 71), 0),
        "block_table": draw_block_table(jax.random.fold_in(key_list[6], 71), 0),
        "lengths": set_ends(jax.random.randint(key_list[4], (BATCH,), BLK, NB * BLK + 1), jax.random.fold_in(key_list[4], 1), BLK, NB * BLK).astype(jnp.int32),
        "output_weight": gaussian(key_list[5], (H * HD, D), (H * HD) ** -0.5, 0.0625, ((0, 4), (1, 8))),
    }


def reference(queries, cache_pool, block_scale, block_table, lengths, output_weight):
    decode_cache = cache_pool[block_table]
    decode_scale = block_scale[block_table]
    groups = H // KVH
    root_scale = 1.0 / math.sqrt(HD)
    offsets = jnp.arange(NB * BLK, dtype=jnp.int32).reshape(NB, BLK)

    def one_request(request_items):
        query_rows, blocks, scales, length = request_items
        key_rows = blocks[:, :, 0].astype(jnp.float32)
        value_rows = blocks[:, :, 1].astype(jnp.float32)
        head_rows = query_rows.reshape(KVH, groups, HD).astype(jnp.float32)
        scores = jnp.einsum('kgd,nktd->nkgt', head_rows, key_rows, precision=lax.Precision.HIGHEST)
        scores = scores * scales[:, :, 0].astype(jnp.float32)[:, :, None, None] * root_scale
        live_mask = (offsets < length)[:, None, None, :]
        scores = jnp.where(live_mask, scores, -jnp.inf)
        peak = lax.optimization_barrier(jnp.max(scores, axis=(0, 3)))
        weight = jnp.where(live_mask, jnp.exp(scores - peak[None, :, :, None]), 0.0)
        denominator = lax.optimization_barrier(jnp.sum(weight, axis=(0, 3)))
        scaled = (weight * scales[:, :, 1].astype(jnp.float32)[:, :, None, None]).astype(jnp.bfloat16)
        numerator = jnp.einsum('nkgt,nktd->kgd', scaled.astype(jnp.float32), value_rows, precision=lax.Precision.HIGHEST)
        return (numerator / denominator[:, :, None]).astype(jnp.bfloat16).reshape(H * HD)
    attended = lax.map(one_request, (queries, decode_cache, decode_scale, lengths))
    attention_output = jnp.dot(attended, output_weight, preferred_element_type=jnp.float32).astype(jnp.bfloat16)
    return (attention_output, decode_cache, decode_scale)
```

```python
import functools
import math

import jax
import jax.numpy as jnp
from jax import lax
from jax.experimental import pallas as pl
from jax.experimental.pallas import tpu as pltpu
from jax.sharding import PartitionSpec as P

MESH = pl.DeviceIdType.MESH
absent_score = -1e30
absent_limit = -1e29


def xor_index(index, mask):
    out = index
    bit = 1
    while bit <= mask:
        if mask & bit:
            out = out + bit - 2 * bit * ((index // bit) % 2)
        bit *= 2
    return out


def exchange_kernel(
    dims,
    lengths_in,
    table_in,
    block_scale_in,
    queries_in,
    pool_ref,
    weight_ref,
    placed_ref,
    scales_out_ref,
    output_ref,
    lengths_ref,
    table_ref,
    block_scale_ref,
    queries_ref,
    raw,
    send,
    arrived,
    weights,
    all_queries,
    scores,
    peaks,
    sums,
    accums,
    parts,
    parts_in,
    stats,
    stats_in,
    attended,
    projected,
    projected_in,
    scales_in,
    scales_wide,
    arrival_rows,
    pick_rows,
    scale_words,
    arrival_words,
    pick_words,
    load_sems,
    local_sems,
    word_sems,
    block_send,
    block_recv,
    query_send,
    query_recv,
    scale_send,
    scale_recv,
    part_send,
    part_recv,
    stat_send,
    stat_recv,
    known_below,
    known_above,
    att_send,
    att_recv,
    proj_send,
    proj_recv,
):
    seq_count, group_count, tp_count, per_group, root_scale = dims
    sources = seq_count * group_count
    seq_index = lax.axis_index("seq")
    group_index = lax.axis_index("grp")
    tp_index = lax.axis_index("tp")
    me = seq_index * group_count + group_index
    planes, _, capacity, block_size, head_size = send.shape
    pool_slots = raw[0].shape[0]
    key_heads = planes // 2
    query_rows = all_queries.shape[2]
    groups = query_rows // per_group
    batch_rows, table_width = table_ref.shape
    share_blocks = table_width // seq_count
    positions = per_group * share_blocks
    row_share = parts.shape[1]
    per_tile = groups // row_share
    f32, bf16 = jnp.float32, jnp.bfloat16

    def pool_load(plane):
        return pltpu.make_async_copy(pool_ref.at[:, plane], raw[plane], load_sems.at[plane])

    table_load = pltpu.make_async_copy(table_in, table_ref, word_sems.at[4])
    small_loads = [
        pltpu.make_async_copy(lengths_in, lengths_ref, word_sems.at[5]),
        pltpu.make_async_copy(block_scale_in, block_scale_ref, word_sems.at[6]),
    ] + [
        pltpu.make_async_copy(
            queries_in.at[request, pl.ds(head * groups, groups)],
            queries_ref.at[head, pl.ds(request * groups, groups)],
            word_sems.at[7 + head * per_group + request],
        )
        for head in range(key_heads)
        for request in range(per_group)
    ]
    table_load.start()
    pool_load(0).start()

    def source_device(other):
        return {"seq": other // group_count, "grp": other % group_count}

    barrier = pltpu.get_barrier_semaphore()
    for step in range(1, sources):
        pl.semaphore_signal(
            barrier, inc=1, device_id=source_device(xor_index(me, step)), device_id_type=MESH
        )
    below, above = tp_index > 0, tp_index < tp_count - 1

    @pl.when(below)
    def _():
        pl.semaphore_signal(
            barrier, inc=1, device_id={"tp": tp_index - 1}, device_id_type=MESH
        )

    @pl.when(above)
    def _():
        pl.semaphore_signal(
            barrier, inc=1, device_id={"tp": tp_index + 1}, device_id_type=MESH
        )

    wide = (batch_rows, table_width)
    table_load.wait()
    table = table_ref[...]
    row_of = lax.broadcasted_iota(jnp.int32, wide, 0)
    col_of = lax.broadcasted_iota(jnp.int32, wide, 1)
    square = (table_width, table_width)
    upper = lax.broadcasted_iota(jnp.int32, square, 0)
    lower = lax.broadcasted_iota(jnp.int32, square, 1)
    alike = upper // share_blocks == lower // share_blocks
    all_alike = jnp.where(alike, 1.0, 0.0).astype(bf16)
    earlier = jnp.where(alike, jnp.where(upper < lower, 1.0, 0.0), 0.0).astype(bf16)
    owner = table // pool_slots
    local = (table % pool_slots).astype(f32)

    def ranks(theirs):
        ones = jnp.where(theirs, 1.0, 0.0).astype(bf16)
        rank = jnp.dot(ones, earlier, preferred_element_type=f32)
        whole = jnp.dot(ones, all_alike, preferred_element_type=f32)
        for request in range(batch_rows):
            last = request // per_group * per_group + per_group
            for later in range(request + 1, last):
                rank = rank + jnp.where(row_of == later, whole[request : request + 1], 0.0)
        return rank

    range_of = jnp.where(upper // share_blocks == lower, 1.0, 0.0).astype(bf16)
    own_rank = jnp.where(owner == me, ranks(owner == me), -1.0)

    def pick(kind, values):
        for within in range(capacity):
            pick_rows[kind, within] = jnp.dot(
                jnp.where(own_rank == within, values, 0.0).astype(bf16),
                range_of,
                preferred_element_type=f32,
            ).astype(jnp.int32)
        return pltpu.make_async_copy(
            pick_rows.at[kind], pick_words.at[kind], word_sems.at[kind]
        )

    slot_copy = pick(0, local)
    slot_copy.start()
    own_queries = pltpu.make_async_copy(queries_ref, all_queries.at[group_index], local_sems.at[0])
    beside = jnp.where(below, 1, 0) + jnp.where(above, 1, 0)
    pl.semaphore_wait(barrier, sources - 1 + beside)

    def query_copy(step):
        return pltpu.make_async_remote_copy(
            src_ref=queries_ref,
            dst_ref=all_queries.at[group_index],
            send_sem=query_send.at[step],
            recv_sem=query_recv.at[step],
            device_id={"grp": xor_index(group_index, step)},
            device_id_type=MESH,
        )

    def scale_copy(step):
        return pltpu.make_async_remote_copy(
            src_ref=block_scale_ref,
            dst_ref=scales_in.at[me],
            send_sem=scale_send.at[step],
            recv_sem=scale_recv.at[step],
            device_id=source_device(xor_index(me, step)),
            device_id_type=MESH,
        )

    own_scales = pltpu.make_async_copy(block_scale_ref, scales_in.at[me], local_sems.at[1])

    def block_copy(plane, step):
        other = xor_index(me, step)
        return pltpu.make_async_remote_copy(
            src_ref=send.at[plane, other],
            dst_ref=arrived[plane].at[pl.ds(me * capacity, capacity)],
            send_sem=block_send.at[plane, step],
            recv_sem=block_recv.at[plane, step],
            device_id=source_device(other),
            device_id_type=MESH,
        )

    def own_blocks(plane):
        return pltpu.make_async_copy(
            send.at[plane, me],
            arrived[plane].at[pl.ds(me * capacity, capacity)],
            local_sems.at[2 + plane],
        )

    steps = sorted(range(1, sources), key=lambda s: (s // group_count == 0, s % group_count, s))

    def picked(kind, other, within, request):
        group = other % group_count
        return pick_words[kind, within, group * per_group + request, other // group_count]

    def slot_of(other, within):
        slot = picked(0, other, within, 0)
        for request in range(1, per_group):
            slot = slot + picked(0, other, within, request)
        return jnp.clip(slot, 0, pool_slots - 1)

    def sort_blocks(plane, other):
        def place(within, _):
            send[plane, other, within] = raw[plane][slot_of(other, within)]
            return 0

        lax.fori_loop(0, capacity, place, 0)

    def sort_plane(plane):
        def place(other, _):
            sort_blocks(plane, other)
            return 0

        lax.fori_loop(0, sources, place, 0)

    def send_plane(plane):
        for step in steps:
            block_copy(plane, step).start()
        own_blocks(plane).start()

    slot_copy.wait()
    pool_load(0).wait()
    for place, step in enumerate(steps):
        sort_blocks(0, xor_index(me, step))
        if place:
            block_copy(0, steps[place - 1]).start()
    sort_blocks(0, me)
    block_copy(0, steps[-1]).start()
    for copy in small_loads:
        copy.start()
    for plane in range(1, planes):
        pool_load(plane).start()
    for copy in small_loads:
        copy.wait()
    own_queries.start()
    for step in range(1, group_count):
        query_copy(step).start()
    for step in steps:
        scale_copy(step).start()
    own_scales.start()
    weight_load = pltpu.make_async_copy(weight_ref, weights, load_sems.at[planes])
    weight_load.start()
    for plane in range(1, planes):
        pool_load(plane).wait()
        sort_plane(plane)
    own_blocks(0).start()

    arrival = jnp.zeros(wide, f32)
    for source in range(sources):
        theirs = owner == source
        arrival = jnp.where(theirs, ranks(theirs) + source * capacity, arrival)
    arrival_rows[...] = arrival.astype(jnp.int32)
    context = jnp.full(wide, lengths_ref[0], jnp.int32)
    for request in range(1, batch_rows):
        context = jnp.where(row_of == request, lengths_ref[request], context)
    live = jnp.clip(context - col_of * block_size, 0, block_size).astype(f32)
    scales_wide[...] = block_scale_ref[...].astype(f32)
    word_copies = [
        pick(1, live),
        pltpu.make_async_copy(arrival_rows, arrival_words, word_sems.at[2]),
        pltpu.make_async_copy(scales_wide, scale_words, word_sems.at[3]),
    ]
    for copy in word_copies:
        copy.start()
    for copy in word_copies:
        copy.wait()

    own_queries.wait()
    for step in range(1, group_count):
        query_copy(step).wait()

    lanes = lax.broadcasted_iota(jnp.int32, (query_rows, block_size), 1)
    row_ids = lax.broadcasted_iota(jnp.int32, (query_rows, block_size), 0)
    share_lanes = lax.broadcasted_iota(jnp.int32, (row_share, head_size), 1)
    share_rows = lax.broadcasted_iota(jnp.int32, (row_share, head_size), 0)
    for head in range(key_heads):
        peaks[...] = jnp.full_like(peaks, absent_score)
        sums[...] = jnp.zeros_like(sums)
        accums[...] = jnp.zeros_like(accums)

        def score_blocks(other, _):
            group = other % group_count
            keys = send[2 * head, other].reshape(capacity * block_size, head_size)
            raw_scores = lax.dot_general(
                all_queries[group, head],
                keys,
                (((1,), (1,)), ((), ())),
                preferred_element_type=jnp.float32,
            )
            highest = peaks[group]
            for within in range(capacity):
                limit = jnp.full(lanes.shape, picked(1, other, within, 0), jnp.int32)
                for request in range(1, per_group):
                    limit = jnp.where(
                        row_ids >= request * groups, picked(1, other, within, request), limit
                    )
                part = raw_scores[:, within * block_size : (within + 1) * block_size]
                part = part * scale_words[2 * head, slot_of(other, within)] * root_scale
                part = jnp.where(lanes < limit, part, absent_score)
                scores[other, :, within * block_size : (within + 1) * block_size] = part
                highest = jnp.maximum(highest, part)
            peaks[group] = highest
            return 0

        lax.fori_loop(0, sources, score_blocks, 0)
        for group in range(group_count):
            peaks[group] = jnp.broadcast_to(
                jnp.max(peaks[group], axis=1, keepdims=True), lanes.shape
            )

        def weigh_blocks(other, _):
            group = other % group_count
            peak = peaks[group]
            total = sums[group]
            pieces = []
            for within in range(capacity):
                part = scores[other, :, within * block_size : (within + 1) * block_size]
                weight = jnp.where(part > absent_limit, jnp.exp(part - peak), 0.0)
                total = total + weight
                pieces.append(
                    (weight * scale_words[2 * head + 1, slot_of(other, within)]).astype(bf16)
                )
            sums[group] = total
            values = send[2 * head + 1, other].reshape(capacity * block_size, head_size)
            accums[group] += jnp.dot(
                jnp.concatenate(pieces, axis=1), values, preferred_element_type=jnp.float32
            )
            return 0

        lax.fori_loop(0, sources, weigh_blocks, 0)
        for group in range(group_count):
            total = jnp.broadcast_to(jnp.sum(sums[group], axis=1, keepdims=True), lanes.shape)
            for request in range(per_group):
                tile = (group * key_heads + head) * per_group + request
                for piece in range(per_tile):
                    low = request * groups + piece * row_share
                    place = tile * per_tile + piece
                    parts[place] = accums[group, low : low + row_share]
                    stats[place] = jnp.sum(
                        jnp.where(
                            share_lanes == share_rows, peaks[group, low : low + row_share], 0.0
                        )
                        + jnp.where(
                            share_lanes == share_rows + row_share,
                            total[low : low + row_share],
                            0.0,
                        ),
                        axis=0,
                        keepdims=True,
                    )

    def part_copy(step):
        other = xor_index(me, step)
        return pltpu.make_async_remote_copy(
            src_ref=parts.at[other],
            dst_ref=parts_in.at[me],
            send_sem=part_send.at[step],
            recv_sem=part_recv.at[step],
            device_id=source_device(other),
            device_id_type=MESH,
        )

    def stat_copy(step):
        other = xor_index(me, step)
        return pltpu.make_async_remote_copy(
            src_ref=stats.at[other],
            dst_ref=stats_in.at[me],
            send_sem=stat_send.at[step],
            recv_sem=stat_recv.at[step],
            device_id=source_device(other),
            device_id_type=MESH,
        )

    for step in steps:
        stat_copy(step).start()
        part_copy(step).start()
    parts_in[me] = parts[me]
    stats_in[me] = stats[me]
    if planes > 1:
        send_plane(1)

    for reach in range(1, tp_count - 1):

        @pl.when(jnp.logical_and(tp_index >= reach, above))
        def _():
            pl.semaphore_signal(
                known_below.at[reach], inc=1, device_id={"tp": tp_index + 1}, device_id_type=MESH
            )

        @pl.when(jnp.logical_and(tp_index + reach < tp_count, below))
        def _():
            pl.semaphore_signal(
                known_above.at[reach], inc=1, device_id={"tp": tp_index - 1}, device_id_type=MESH
            )

        @pl.when(tp_index - 1 >= reach)
        def _():
            pl.semaphore_wait(known_below.at[reach], 1)

        @pl.when(tp_index + 1 + reach < tp_count)
        def _():
            pl.semaphore_wait(known_above.at[reach], 1)

    for step in steps:
        stat_copy(step).wait_recv()
        part_copy(step).wait_recv()

    def spread(source, first):
        return jnp.broadcast_to(
            jnp.sum(
                jnp.where(
                    share_lanes == share_rows + first,
                    jnp.broadcast_to(stats_in[source], share_lanes.shape),
                    0.0,
                ),
                axis=1,
                keepdims=True,
            ),
            share_lanes.shape,
        )

    source_peaks = [spread(source, 0) for source in range(sources)]
    highest = functools.reduce(jnp.maximum, source_peaks)
    numerator = jnp.zeros_like(highest)
    denominator = jnp.zeros_like(highest)
    for source in range(sources):
        factor = jnp.exp(source_peaks[source] - highest)
        numerator += parts_in[source] * factor
        denominator += spread(source, row_share) * factor
    attended[me] = (numerator / denominator).astype(jnp.bfloat16)

    def att_copy(step):
        return pltpu.make_async_remote_copy(
            src_ref=attended.at[me],
            dst_ref=attended.at[me],
            send_sem=att_send.at[step],
            recv_sem=att_recv.at[step],
            device_id=source_device(xor_index(me, step)),
            device_id_type=MESH,
        )

    weight_load.wait()
    for step in steps:
        att_copy(step).start()
    for plane in range(2, planes):
        send_plane(plane)
    for step in steps:
        att_copy(step).wait_recv()

    rows = sources * row_share
    gathered = attended[...].astype(f32).reshape(rows, head_size)
    row = lax.broadcasted_iota(jnp.int32, (rows, head_size), 0)
    row_head = (row // (groups * per_group)) % key_heads * groups + row % groups
    left = jnp.concatenate(
        [
            jnp.where(row_head == head, gathered, 0.0).astype(jnp.bfloat16)
            for head in range(key_heads * groups)
        ],
        axis=1,
    )
    columns = weights.shape[1]
    width = min(columns, 256)
    here = batch_rows // tp_count
    for low in range(0, columns, width):
        product = jnp.dot(left, weights[:, low : low + width], preferred_element_type=jnp.float32)
        for request in range(batch_rows):
            group, inner = request // per_group, request % per_group
            total = jnp.zeros((1, width), jnp.float32)
            for head in range(key_heads):
                tile = (group * key_heads + head) * per_group + inner
                total += jnp.sum(
                    product[tile * groups : (tile + 1) * groups], axis=0, keepdims=True
                )
            projected[request // here, pl.ds(request % here, 1), low : low + width] = total

    def proj_copy(step):
        other = xor_index(tp_index, step)
        return pltpu.make_async_remote_copy(
            src_ref=projected.at[other],
            dst_ref=projected_in.at[tp_index],
            send_sem=proj_send.at[step],
            recv_sem=proj_recv.at[step],
            device_id={"tp": other},
            device_id_type=MESH,
        )

    for step in range(1, tp_count):
        proj_copy(step).start()
    projected_in[tp_index] = projected[tp_index]
    for step in range(1, tp_count):
        proj_copy(step).wait()
    total = projected_in[0]
    for source in range(1, tp_count):
        total += projected_in[source]
    output_ref[...] = total.astype(output_ref.dtype)

    own_scales.wait()
    for step in steps:
        scale_copy(step).wait()
    slot_ids = lax.broadcasted_iota(jnp.int32, (pool_slots, table_width), 0)
    wanted = jnp.where(
        lax.broadcasted_iota(jnp.int32, (table_width, share_blocks), 0)
        == lax.broadcasted_iota(jnp.int32, (table_width, share_blocks), 1)
        + seq_index * share_blocks,
        1.0,
        0.0,
    ).astype(bf16)
    for request in range(per_group):
        slots = table_ref[pl.ds(group_index * per_group + request, 1), :]
        found = jnp.zeros((planes, table_width), f32)
        for source in range(sources):
            onehot = jnp.where(slots == slot_ids + source * pool_slots, 1.0, 0.0).astype(bf16)
            found += jnp.dot(scales_in[source], onehot, preferred_element_type=f32)
        scales_out_ref[request] = jnp.dot(
            found.astype(bf16), wanted, preferred_element_type=f32
        ).astype(bf16)

    unroll = 4 if share_blocks % 4 == 0 else 1
    for plane in range(planes):
        own_blocks(plane).wait()
        for step in steps:
            block_copy(plane, step).wait_recv()
        for request in range(per_group):

            def place(turn, _):
                for part in range(unroll):
                    column = turn * unroll + part
                    index = arrival_words[
                        group_index * per_group + request, seq_index * share_blocks + column
                    ]
                    placed_ref[request * share_blocks + column, plane] = arrived[plane][
                        jnp.clip(index, 0, positions - 1)
                    ]
                return 0

            lax.fori_loop(0, share_blocks // unroll, place, 0)
    for step in steps:
        part_copy(step).wait_send()
        stat_copy(step).wait_send()
        att_copy(step).wait_send()
        for plane in range(planes):
            block_copy(plane, step).wait_send()


def copy_out_kernel(cache_in, scale_in, output_in, cache_ref, scale_ref, output_ref, sems):
    share = cache_in.shape[0] // 4
    copies = [
        pltpu.make_async_copy(
            cache_in.at[pl.ds(part * share, share)],
            cache_ref.at[pl.ds(part * share, share)],
            sems.at[part],
        )
        for part in range(4)
    ]
    copies.append(pltpu.make_async_copy(scale_in, scale_ref, sems.at[4]))
    copies.append(pltpu.make_async_copy(output_in, output_ref, sems.at[5]))
    for copy in copies:
        copy.start()
    for copy in copies:
        copy.wait()


def per_device(queries, cache_pool, block_scale, block_table, lengths, output_weight):
    seq_count = lax.axis_size("seq")
    group_count = lax.axis_size("grp")
    tp_count = lax.axis_size("tp")
    sources = seq_count * group_count
    pool_slots, key_heads, _, block_size, head_size = cache_pool.shape
    batch_rows, table_width = block_table.shape
    per_group = batch_rows // group_count
    share_blocks = table_width // seq_count
    capacity = pool_slots // sources
    heads_here = queries.shape[1]
    groups = heads_here // key_heads
    planes = key_heads * 2
    positions = per_group * share_blocks
    columns = output_weight.shape[1]
    root_scale = 1.0 / math.sqrt(head_size)

    row_share = batch_rows * key_heads * groups // sources
    query_rows = per_group * groups
    f32, bf16 = jnp.float32, jnp.bfloat16
    dma = pltpu.SemaphoreType.DMA
    vmem = pl.BlockSpec(memory_space=pltpu.VMEM)
    hbm = pl.BlockSpec(memory_space=pltpu.HBM)
    here = batch_rows // tp_count
    decode_cache, decode_scale, output = pl.pallas_call(
        functools.partial(
            exchange_kernel, (seq_count, group_count, tp_count, per_group, root_scale)
        ),
        out_shape=(
            pltpu.VMEM((positions, planes, block_size, head_size), bf16),
            pltpu.VMEM((per_group, planes, share_blocks), bf16),
            pltpu.VMEM((here, columns), bf16),
        ),
        in_specs=[hbm, hbm, hbm, hbm, hbm, hbm],
        out_specs=(vmem, vmem, vmem),
        scratch_shapes=[
            pltpu.SMEM((batch_rows,), jnp.int32),
            pltpu.VMEM((batch_rows, table_width), jnp.int32),
            pltpu.VMEM((planes, pool_slots), bf16),
            pltpu.VMEM((key_heads, query_rows, head_size), bf16),
            [pltpu.VMEM((pool_slots, block_size, head_size), bf16) for _ in range(planes)],
            pltpu.VMEM((planes, sources, capacity, block_size, head_size), bf16),
            [pltpu.VMEM((pool_slots, block_size, head_size), bf16) for _ in range(planes)],
            pltpu.VMEM((heads_here * head_size, columns), bf16),
            pltpu.VMEM((group_count, key_heads, query_rows, head_size), bf16),
            pltpu.VMEM((sources, query_rows, capacity * block_size), f32),
            pltpu.VMEM((group_count, query_rows, block_size), f32),
            pltpu.VMEM((group_count, query_rows, block_size), f32),
            pltpu.VMEM((group_count, query_rows, head_size), f32),
            pltpu.VMEM((sources, row_share, head_size), f32),
            pltpu.VMEM((sources, row_share, head_size), f32),
            pltpu.VMEM((sources, 1, head_size), f32),
            pltpu.VMEM((sources, 1, head_size), f32),
            pltpu.VMEM((sources, row_share, head_size), bf16),
            pltpu.VMEM((tp_count, here, columns), f32),
            pltpu.VMEM((tp_count, here, columns), f32),
            pltpu.VMEM((sources, planes, pool_slots), bf16),
            pltpu.VMEM((planes, pool_slots), f32),
            pltpu.VMEM((batch_rows, table_width), jnp.int32),
            pltpu.VMEM((2, capacity, batch_rows, table_width), jnp.int32),
            pltpu.SMEM((planes, pool_slots), f32),
            pltpu.SMEM((batch_rows, table_width), jnp.int32),
            pltpu.SMEM((2, capacity, batch_rows, table_width), jnp.int32),
            dma((planes + 1,)),
            dma((planes + 3,)),
            dma((7 + key_heads * per_group,)),
            dma((planes, sources)),
            dma((planes, sources)),
            dma((group_count,)),
            dma((group_count,)),
            dma((sources,)),
            dma((sources,)),
            dma((sources,)),
            dma((sources,)),
            dma((sources,)),
            dma((sources,)),
            pltpu.SemaphoreType.REGULAR((tp_count,)),
            pltpu.SemaphoreType.REGULAR((tp_count,)),
            dma((sources,)),
            dma((sources,)),
            dma((tp_count,)),
            dma((tp_count,)),
        ],
        compiler_params=pltpu.CompilerParams(
            collective_id=0, has_side_effects=True, vmem_limit_bytes=40 * 2**20
        ),
    )(
        *(
            pltpu.with_memory_space_constraint(operand, pltpu.HBM)
            for operand in (
                lengths,
                block_table,
                block_scale.reshape(pool_slots, planes).T,
                queries,
                cache_pool.reshape(pool_slots, planes, block_size, head_size),
                output_weight,
            )
        )
    )
    results = (decode_cache, decode_scale, output)
    decode_cache, decode_scale, output = pl.pallas_call(
        copy_out_kernel,
        out_shape=tuple(jax.ShapeDtypeStruct(r.shape, r.dtype) for r in results),
        in_specs=[vmem] * 3,
        out_specs=(hbm,) * 3,
        scratch_shapes=[dma((6,))],
        compiler_params=pltpu.CompilerParams(vmem_limit_bytes=16 * 2**20),
    )(*(pltpu.with_memory_space_constraint(r, pltpu.VMEM) for r in results))
    return (
        output,
        decode_cache.reshape(per_group, share_blocks, key_heads, 2, block_size, head_size),
        decode_scale.transpose(0, 2, 1).reshape(per_group, share_blocks, key_heads, 2),
    )


def solution(mesh):
    placed = (
        P("grp", "tp", None),
        P(("seq", "grp"), "tp", None, None, None),
        P(("seq", "grp"), "tp", None),
        P(),
        P(),
        P("tp", ("seq", "grp")),
    )
    return jax.shard_map(
        per_device,
        mesh=mesh,
        in_specs=placed,
        out_specs=(
            P("tp", ("seq", "grp")),
            P("grp", "seq", "tp", None, None, None),
            P("grp", "seq", "tp", None),
        ),
        check_vma=False,
    )
```

```python
import functools
import math

import jax
import jax.numpy as jnp
from jax import lax
from jax.experimental import pallas as pl
from jax.experimental.pallas import tpu as pltpu
from jax.sharding import PartitionSpec as P

MESH = pl.DeviceIdType.MESH
absent_score = -1e30
absent_limit = -1e29


def xor_index(index, mask):
    out = index
    bit = 1
    while bit <= mask:
        if mask & bit:
            out = out + bit - 2 * bit * ((index // bit) % 2)
        bit *= 2
    return out


def exchange_kernel(
    dims,
    lengths_in,
    table_in,
    block_scale_in,
    queries_in,
    pool_ref,
    weight_ref,
    placed_ref,
    last_ref,
    arrival_rows,
    scales_out_ref,
    output_ref,
    lengths_ref,
    table_ref,
    block_scale_ref,
    queries_ref,
    raw,
    send,
    arrived,
    weights,
    all_queries,
    scores,
    peaks,
    sums,
    accums,
    parts,
    parts_in,
    stats,
    stats_in,
    attended,
    projected,
    projected_in,
    scales_in,
    scales_wide,
    pick_rows,
    scale_words,
    arrival_words,
    pick_words,
    load_sems,
    local_sems,
    word_sems,
    block_send,
    block_recv,
    query_send,
    query_recv,
    scale_send,
    scale_recv,
    part_send,
    part_recv,
    stat_send,
    stat_recv,
    known_below,
    known_above,
    att_send,
    att_recv,
    proj_send,
    proj_recv,
):
    seq_count, group_count, tp_count, per_group, root_scale = dims
    sources = seq_count * group_count
    seq_index = lax.axis_index("seq")
    group_index = lax.axis_index("grp")
    tp_index = lax.axis_index("tp")
    me = seq_index * group_count + group_index
    planes, _, capacity, block_size, head_size = send.shape
    arrived = [*arrived, last_ref]
    pool_slots = raw[0].shape[0]
    key_heads = planes // 2
    query_rows = all_queries.shape[2]
    groups = query_rows // per_group
    batch_rows, table_width = table_ref.shape
    share_blocks = table_width // seq_count
    positions = per_group * share_blocks
    row_share = parts.shape[1]
    per_tile = groups // row_share
    f32, bf16 = jnp.float32, jnp.bfloat16

    def pool_load(plane):
        return pltpu.make_async_copy(pool_ref.at[:, plane], raw[plane], load_sems.at[plane])

    table_load = pltpu.make_async_copy(table_in, table_ref, word_sems.at[4])
    small_loads = [
        pltpu.make_async_copy(lengths_in, lengths_ref, word_sems.at[5]),
        pltpu.make_async_copy(block_scale_in, block_scale_ref, word_sems.at[6]),
    ] + [
        pltpu.make_async_copy(
            queries_in.at[request, pl.ds(head * groups, groups)],
            queries_ref.at[head, pl.ds(request * groups, groups)],
            word_sems.at[7 + head * per_group + request],
        )
        for head in range(key_heads)
        for request in range(per_group)
    ]
    table_load.start()
    pool_load(0).start()

    def source_device(other):
        return {"seq": other // group_count, "grp": other % group_count}

    barrier = pltpu.get_barrier_semaphore()
    for step in range(1, sources):
        pl.semaphore_signal(
            barrier, inc=1, device_id=source_device(xor_index(me, step)), device_id_type=MESH
        )
    below, above = tp_index > 0, tp_index < tp_count - 1

    @pl.when(above)
    def _():
        pl.semaphore_signal(
            barrier, inc=1, device_id={"tp": tp_index + 1}, device_id_type=MESH
        )

    wide = (batch_rows, table_width)
    table_load.wait()
    table = table_ref[...]
    row_of = lax.broadcasted_iota(jnp.int32, wide, 0)
    col_of = lax.broadcasted_iota(jnp.int32, wide, 1)
    square = (table_width, table_width)
    upper = lax.broadcasted_iota(jnp.int32, square, 0)
    lower = lax.broadcasted_iota(jnp.int32, square, 1)
    alike = upper // share_blocks == lower // share_blocks
    all_alike = jnp.where(alike, 1.0, 0.0).astype(bf16)
    earlier = jnp.where(alike, jnp.where(upper < lower, 1.0, 0.0), 0.0).astype(bf16)
    owner = table // pool_slots
    local = (table % pool_slots).astype(f32)

    def ranks(theirs):
        ones = jnp.where(theirs, 1.0, 0.0).astype(bf16)
        rank = jnp.dot(ones, earlier, preferred_element_type=f32)
        whole = jnp.dot(ones, all_alike, preferred_element_type=f32)
        for request in range(batch_rows):
            last = request // per_group * per_group + per_group
            for later in range(request + 1, last):
                rank = rank + jnp.where(row_of == later, whole[request : request + 1], 0.0)
        return rank

    range_of = jnp.where(upper // share_blocks == lower, 1.0, 0.0).astype(bf16)
    own_rank = jnp.where(owner == me, ranks(owner == me), -1.0)

    def pick(kind, values):
        for within in range(capacity):
            pick_rows[kind, within] = jnp.dot(
                jnp.where(own_rank == within, values, 0.0).astype(bf16),
                range_of,
                preferred_element_type=f32,
            ).astype(jnp.int32)
        return pltpu.make_async_copy(
            pick_rows.at[kind], pick_words.at[kind], word_sems.at[kind]
        )

    slot_copy = pick(0, local)
    slot_copy.start()
    own_queries = pltpu.make_async_copy(queries_ref, all_queries.at[group_index], local_sems.at[0])
    pl.semaphore_wait(barrier, sources - 1 + jnp.where(below, 1, 0))

    def query_copy(step):
        return pltpu.make_async_remote_copy(
            src_ref=queries_ref,
            dst_ref=all_queries.at[group_index],
            send_sem=query_send.at[step],
            recv_sem=query_recv.at[step],
            device_id={"grp": xor_index(group_index, step)},
            device_id_type=MESH,
        )

    def scale_copy(step):
        return pltpu.make_async_remote_copy(
            src_ref=block_scale_ref,
            dst_ref=scales_in.at[me],
            send_sem=scale_send.at[step],
            recv_sem=scale_recv.at[step],
            device_id=source_device(xor_index(me, step)),
            device_id_type=MESH,
        )

    own_scales = pltpu.make_async_copy(block_scale_ref, scales_in.at[me], local_sems.at[1])

    def block_copy(plane, step):
        other = xor_index(me, step)
        return pltpu.make_async_remote_copy(
            src_ref=send.at[plane, other],
            dst_ref=arrived[plane].at[pl.ds(me * capacity, capacity)],
            send_sem=block_send.at[plane, step],
            recv_sem=block_recv.at[plane, step],
            device_id=source_device(other),
            device_id_type=MESH,
        )

    def own_blocks(plane):
        return pltpu.make_async_copy(
            send.at[plane, me],
            arrived[plane].at[pl.ds(me * capacity, capacity)],
            local_sems.at[2 + plane],
        )

    steps = sorted(range(1, sources), key=lambda s: (s // group_count == 0, s % group_count, s))
    near_steps = [s for s in steps if (s // group_count).bit_count() <= 1]
    far_steps = [s for s in steps if s not in near_steps]

    def picked(kind, other, within, request):
        group = other % group_count
        return pick_words[kind, within, group * per_group + request, other // group_count]

    def slot_of(other, within):
        slot = picked(0, other, within, 0)
        for request in range(1, per_group):
            slot = slot + picked(0, other, within, request)
        return jnp.clip(slot, 0, pool_slots - 1)

    def sort_blocks(plane, other):
        def place(within, _):
            send[plane, other, within] = raw[plane][slot_of(other, within)]
            return 0

        lax.fori_loop(0, capacity, place, 0)

    def sort_plane(plane):
        def place(other, _):
            sort_blocks(plane, other)
            return 0

        lax.fori_loop(0, sources, place, 0)

    def send_plane(plane, chosen):
        for step in chosen:
            block_copy(plane, step).start()

    slot_copy.wait()
    pool_load(0).wait()
    for place, step in enumerate(near_steps):
        other = xor_index(me, step)
        for within in range(capacity):
            send[0, other, within] = raw[0][slot_of(other, within)]
        if place:
            block_copy(0, near_steps[place - 1]).start()
    sort_blocks(0, me)
    block_copy(0, near_steps[-1]).start()
    for copy in small_loads:
        copy.start()
    for plane in range(1, planes):
        pool_load(plane).start()
    for copy in small_loads:
        copy.wait()
    own_queries.start()
    for step in range(1, group_count):
        query_copy(step).start()
    for step in steps:
        scale_copy(step).start()
    own_scales.start()
    weight_load = pltpu.make_async_copy(weight_ref, weights, load_sems.at[planes])
    weight_load.start()
    for step in far_steps:
        sort_blocks(0, xor_index(me, step))
    for plane in range(1, planes):
        pool_load(plane).wait()
        sort_plane(plane)
        if plane == 1:
            send_plane(plane, near_steps)
    for plane in range(planes):
        own_blocks(plane).start()

    arrival = jnp.zeros(wide, f32)
    for source in range(sources):
        theirs = owner == source
        arrival = jnp.where(theirs, ranks(theirs) + source * capacity, arrival)
    arrival_rows[...] = arrival.astype(jnp.int32)
    context = jnp.full(wide, lengths_ref[0], jnp.int32)
    for request in range(1, batch_rows):
        context = jnp.where(row_of == request, lengths_ref[request], context)
    live = jnp.clip(context - col_of * block_size, 0, block_size).astype(f32)
    scales_wide[...] = block_scale_ref[...].astype(f32)
    word_copies = [
        pick(1, live),
        pltpu.make_async_copy(arrival_rows, arrival_words, word_sems.at[2]),
        pltpu.make_async_copy(scales_wide, scale_words, word_sems.at[3]),
    ]
    for copy in word_copies:
        copy.start()
    for copy in word_copies:
        copy.wait()

    own_queries.wait()
    for step in range(1, group_count):
        query_copy(step).wait()

    lanes = lax.broadcasted_iota(jnp.int32, (query_rows, block_size), 1)
    row_ids = lax.broadcasted_iota(jnp.int32, (query_rows, block_size), 0)
    share_lanes = lax.broadcasted_iota(jnp.int32, (row_share, head_size), 1)
    share_rows = lax.broadcasted_iota(jnp.int32, (row_share, head_size), 0)
    for head in range(key_heads):
        peaks[...] = jnp.full_like(peaks, absent_score)
        sums[...] = jnp.zeros_like(sums)
        accums[...] = jnp.zeros_like(accums)

        def score_blocks(other, _):
            group = other % group_count
            keys = send[2 * head, other].reshape(capacity * block_size, head_size)
            raw_scores = lax.dot_general(
                all_queries[group, head],
                keys,
                (((1,), (1,)), ((), ())),
                preferred_element_type=jnp.float32,
            )
            highest = peaks[group]
            for within in range(capacity):
                limit = jnp.full(lanes.shape, picked(1, other, within, 0), jnp.int32)
                for request in range(1, per_group):
                    limit = jnp.where(
                        row_ids >= request * groups, picked(1, other, within, request), limit
                    )
                part = raw_scores[:, within * block_size : (within + 1) * block_size]
                part = part * scale_words[2 * head, slot_of(other, within)] * root_scale
                part = jnp.where(lanes < limit, part, absent_score)
                scores[other, :, within * block_size : (within + 1) * block_size] = part
                highest = jnp.maximum(highest, part)
            peaks[group] = highest
            return 0

        lax.fori_loop(0, sources, score_blocks, 0)
        for group in range(group_count):
            peaks[group] = jnp.broadcast_to(
                jnp.max(peaks[group], axis=1, keepdims=True), lanes.shape
            )

        def weigh_blocks(other, _):
            group = other % group_count
            peak = peaks[group]
            total = sums[group]
            pieces = []
            for within in range(capacity):
                part = scores[other, :, within * block_size : (within + 1) * block_size]
                weight = jnp.where(part > absent_limit, jnp.exp(part - peak), 0.0)
                total = total + weight
                pieces.append(
                    (weight * scale_words[2 * head + 1, slot_of(other, within)]).astype(bf16)
                )
            sums[group] = total
            values = send[2 * head + 1, other].reshape(capacity * block_size, head_size)
            accums[group] += jnp.dot(
                jnp.concatenate(pieces, axis=1), values, preferred_element_type=jnp.float32
            )
            return 0

        lax.fori_loop(0, sources, weigh_blocks, 0)
        for group in range(group_count):
            total = jnp.broadcast_to(jnp.sum(sums[group], axis=1, keepdims=True), lanes.shape)
            for request in range(per_group):
                tile = (group * key_heads + head) * per_group + request
                for piece in range(per_tile):
                    low = request * groups + piece * row_share
                    place = tile * per_tile + piece
                    parts[place] = accums[group, low : low + row_share].astype(bf16)
                    stats[place] = jnp.sum(
                        jnp.where(
                            share_lanes == share_rows, peaks[group, low : low + row_share], 0.0
                        )
                        + jnp.where(
                            share_lanes == share_rows + row_share,
                            total[low : low + row_share],
                            0.0,
                        ),
                        axis=0,
                        keepdims=True,
                    )

    def part_copy(step):
        other = xor_index(me, step)
        return pltpu.make_async_remote_copy(
            src_ref=parts.at[other],
            dst_ref=parts_in.at[me],
            send_sem=part_send.at[step],
            recv_sem=part_recv.at[step],
            device_id=source_device(other),
            device_id_type=MESH,
        )

    def stat_copy(step):
        other = xor_index(me, step)
        return pltpu.make_async_remote_copy(
            src_ref=stats.at[other],
            dst_ref=stats_in.at[me],
            send_sem=stat_send.at[step],
            recv_sem=stat_recv.at[step],
            device_id=source_device(other),
            device_id_type=MESH,
        )

    for step in steps:
        stat_copy(step).start()
        part_copy(step).start()
    parts_in[me] = parts[me]
    stats_in[me] = stats[me]
    for plane in range(2, min(planes, 3)):
        send_plane(plane, near_steps)

    @pl.when(below)
    def _():
        pl.semaphore_signal(
            known_above.at[0], inc=1, device_id={"tp": tp_index - 1}, device_id_type=MESH
        )

    @pl.when(above)
    def _():
        pl.semaphore_wait(known_above.at[0], 1)

    for reach in range(1, tp_count - 1):

        @pl.when(jnp.logical_and(tp_index >= reach, above))
        def _():
            pl.semaphore_signal(
                known_below.at[reach], inc=1, device_id={"tp": tp_index + 1}, device_id_type=MESH
            )

        @pl.when(jnp.logical_and(tp_index + reach < tp_count, below))
        def _():
            pl.semaphore_signal(
                known_above.at[reach], inc=1, device_id={"tp": tp_index - 1}, device_id_type=MESH
            )

        @pl.when(tp_index - 1 >= reach)
        def _():
            pl.semaphore_wait(known_below.at[reach], 1)

        @pl.when(tp_index + 1 + reach < tp_count)
        def _():
            pl.semaphore_wait(known_above.at[reach], 1)

    for step in steps:
        stat_copy(step).wait_recv()
        part_copy(step).wait_recv()

    def spread(source, first):
        return jnp.broadcast_to(
            jnp.sum(
                jnp.where(
                    share_lanes == share_rows + first,
                    jnp.broadcast_to(stats_in[source], share_lanes.shape),
                    0.0,
                ),
                axis=1,
                keepdims=True,
            ),
            share_lanes.shape,
        )

    source_peaks = [spread(source, 0) for source in range(sources)]
    highest = functools.reduce(jnp.maximum, source_peaks)
    numerator = jnp.zeros_like(highest)
    denominator = jnp.zeros_like(highest)
    for source in range(sources):
        factor = jnp.exp(source_peaks[source] - highest)
        numerator += parts_in[source].astype(f32) * factor
        denominator += spread(source, row_share) * factor
    attended[me] = (numerator / denominator).astype(jnp.bfloat16)

    def att_copy(step):
        return pltpu.make_async_remote_copy(
            src_ref=attended.at[me],
            dst_ref=attended.at[me],
            send_sem=att_send.at[step],
            recv_sem=att_recv.at[step],
            device_id=source_device(xor_index(me, step)),
            device_id_type=MESH,
        )

    weight_load.wait()
    for step in steps:
        att_copy(step).start()
    for plane in range(3, planes):
        send_plane(plane, near_steps)
    for step in steps:
        att_copy(step).wait_recv()
    for plane in range(planes):
        for step in near_steps:
            block_copy(plane, step).wait_send()
    for plane in range(planes):
        send_plane(plane, far_steps)

    rows = sources * row_share
    gathered = attended[...].astype(f32).reshape(rows, head_size)
    row = lax.broadcasted_iota(jnp.int32, (rows, head_size), 0)
    row_head = (row // (groups * per_group)) % key_heads * groups + row % groups
    left = jnp.concatenate(
        [
            jnp.where(row_head == head, gathered, 0.0).astype(jnp.bfloat16)
            for head in range(key_heads * groups)
        ],
        axis=1,
    )
    columns = weights.shape[1]
    width = min(columns, 256)
    here = batch_rows // tp_count
    for low in range(0, columns, width):
        product = jnp.dot(left, weights[:, low : low + width], preferred_element_type=jnp.float32)
        for request in range(batch_rows):
            group, inner = request // per_group, request % per_group
            total = jnp.zeros((1, width), jnp.float32)
            for head in range(key_heads):
                tile = (group * key_heads + head) * per_group + inner
                total += jnp.sum(
                    product[tile * groups : (tile + 1) * groups], axis=0, keepdims=True
                )
            projected[request // here, pl.ds(request % here, 1), low : low + width] = total

    def proj_copy(step):
        other = xor_index(tp_index, step)
        return pltpu.make_async_remote_copy(
            src_ref=projected.at[other],
            dst_ref=projected_in.at[tp_index],
            send_sem=proj_send.at[step],
            recv_sem=proj_recv.at[step],
            device_id={"tp": other},
            device_id_type=MESH,
        )

    for step in range(1, tp_count):
        proj_copy(step).start()
    projected_in[tp_index] = projected[tp_index]
    for step in range(1, tp_count):
        proj_copy(step).wait()
    total = projected_in[0]
    for source in range(1, tp_count):
        total += projected_in[source]
    output_ref[...] = total.astype(output_ref.dtype)

    own_scales.wait()
    for step in steps:
        scale_copy(step).wait()
    slot_ids = lax.broadcasted_iota(jnp.int32, (pool_slots, table_width), 0)
    wanted = jnp.where(
        lax.broadcasted_iota(jnp.int32, (table_width, share_blocks), 0)
        == lax.broadcasted_iota(jnp.int32, (table_width, share_blocks), 1)
        + seq_index * share_blocks,
        1.0,
        0.0,
    ).astype(bf16)
    for request in range(per_group):
        slots = table_ref[pl.ds(group_index * per_group + request, 1), :]
        found = jnp.zeros((planes, table_width), f32)
        for source in range(sources):
            onehot = jnp.where(slots == slot_ids + source * pool_slots, 1.0, 0.0).astype(bf16)
            found += jnp.dot(scales_in[source], onehot, preferred_element_type=f32)
        scales_out_ref[request] = jnp.dot(
            found.astype(bf16), wanted, preferred_element_type=f32
        ).astype(bf16)

    unroll = 4 if share_blocks % 4 == 0 else 1
    for plane in range(planes - 1):
        own_blocks(plane).wait()
        for step in steps:
            block_copy(plane, step).wait_recv()
        for request in range(per_group):

            def place(turn, _):
                for part in range(unroll):
                    column = turn * unroll + part
                    index = arrival_words[
                        group_index * per_group + request, seq_index * share_blocks + column
                    ]
                    placed_ref[request * share_blocks + column, plane] = arrived[plane][
                        jnp.clip(index, 0, positions - 1)
                    ]
                return 0

            lax.fori_loop(0, share_blocks // unroll, place, 0)
    for step in steps:
        part_copy(step).wait_send()
        stat_copy(step).wait_send()
        att_copy(step).wait_send()
    own_blocks(planes - 1).wait()
    for step in near_steps:
        block_copy(planes - 1, step).wait_recv()
    for plane in range(planes):
        for step in far_steps:
            block_copy(plane, step).wait_send()
    for step in far_steps:
        block_copy(planes - 1, step).wait_recv()


def copy_out_kernel(
    placed_in,
    last_in,
    arrival_in,
    scale_in,
    output_in,
    cache_ref,
    scale_ref,
    output_ref,
    arrival_words,
    sems,
    block_sem,
):
    positions, first = placed_in.shape[:2]
    per_group, _, share_blocks = scale_in.shape
    group_index, seq_index = lax.axis_index("grp"), lax.axis_index("seq")
    words = pltpu.make_async_copy(arrival_in, arrival_words, sems.at[0])
    words.start()
    chunks = 8
    share = positions // chunks
    copies = [
        pltpu.make_async_copy(
            placed_in.at[pl.ds(part * share, share)],
            cache_ref.at[pl.ds(part * share, share), pl.ds(0, first)],
            sems.at[3 + part],
        )
        for part in range(chunks)
    ]
    copies.append(pltpu.make_async_copy(scale_in, scale_ref, sems.at[1]))
    copies.append(pltpu.make_async_copy(output_in, output_ref, sems.at[2]))
    for copy in copies:
        copy.start()
    words.wait()

    def block(position):
        index = arrival_words[
            group_index * per_group + position // share_blocks,
            seq_index * share_blocks + position % share_blocks,
        ]
        return pltpu.make_async_copy(
            last_in.at[jnp.clip(index, 0, positions - 1)],
            cache_ref.at[position, first],
            block_sem,
        )

    def start(position, _):
        block(position).start()
        return 0

    lax.fori_loop(0, positions, start, 0, unroll=4)
    for copy in copies:
        copy.wait()
    pltpu.make_async_copy(last_in, cache_ref.at[:, first], block_sem).wait()


def per_device(queries, cache_pool, block_scale, block_table, lengths, output_weight):
    seq_count = lax.axis_size("seq")
    group_count = lax.axis_size("grp")
    tp_count = lax.axis_size("tp")
    sources = seq_count * group_count
    pool_slots, key_heads, _, block_size, head_size = cache_pool.shape
    batch_rows, table_width = block_table.shape
    per_group = batch_rows // group_count
    share_blocks = table_width // seq_count
    capacity = pool_slots // sources
    heads_here = queries.shape[1]
    groups = heads_here // key_heads
    planes = key_heads * 2
    positions = per_group * share_blocks
    columns = output_weight.shape[1]
    root_scale = 1.0 / math.sqrt(head_size)

    row_share = batch_rows * key_heads * groups // sources
    query_rows = per_group * groups
    f32, bf16 = jnp.float32, jnp.bfloat16
    dma = pltpu.SemaphoreType.DMA
    vmem = pl.BlockSpec(memory_space=pltpu.VMEM)
    hbm = pl.BlockSpec(memory_space=pltpu.HBM)
    here = batch_rows // tp_count
    results = pl.pallas_call(
        functools.partial(
            exchange_kernel, (seq_count, group_count, tp_count, per_group, root_scale)
        ),
        out_shape=(
            pltpu.VMEM((positions, planes - 1, block_size, head_size), bf16),
            pltpu.VMEM((positions, block_size, head_size), bf16),
            pltpu.VMEM((batch_rows, table_width), jnp.int32),
            pltpu.VMEM((per_group, planes, share_blocks), bf16),
            pltpu.VMEM((here, columns), bf16),
        ),
        in_specs=[hbm, hbm, hbm, hbm, hbm, hbm],
        out_specs=(vmem,) * 5,
        scratch_shapes=[
            pltpu.SMEM((batch_rows,), jnp.int32),
            pltpu.VMEM((batch_rows, table_width), jnp.int32),
            pltpu.VMEM((planes, pool_slots), bf16),
            pltpu.VMEM((key_heads, query_rows, head_size), bf16),
            [pltpu.VMEM((pool_slots, block_size, head_size), bf16) for _ in range(planes)],
            pltpu.VMEM((planes, sources, capacity, block_size, head_size), bf16),
            [pltpu.VMEM((pool_slots, block_size, head_size), bf16) for _ in range(planes - 1)],
            pltpu.VMEM((heads_here * head_size, columns), bf16),
            pltpu.VMEM((group_count, key_heads, query_rows, head_size), bf16),
            pltpu.VMEM((sources, query_rows, capacity * block_size), f32),
            pltpu.VMEM((group_count, query_rows, block_size), f32),
            pltpu.VMEM((group_count, query_rows, block_size), f32),
            pltpu.VMEM((group_count, query_rows, head_size), f32),
            pltpu.VMEM((sources, row_share, head_size), bf16),
            pltpu.VMEM((sources, row_share, head_size), bf16),
            pltpu.VMEM((sources, 1, head_size), f32),
            pltpu.VMEM((sources, 1, head_size), f32),
            pltpu.VMEM((sources, row_share, head_size), bf16),
            pltpu.VMEM((tp_count, here, columns), f32),
            pltpu.VMEM((tp_count, here, columns), f32),
            pltpu.VMEM((sources, planes, pool_slots), bf16),
            pltpu.VMEM((planes, pool_slots), f32),
            pltpu.VMEM((2, capacity, batch_rows, table_width), jnp.int32),
            pltpu.SMEM((planes, pool_slots), f32),
            pltpu.SMEM((batch_rows, table_width), jnp.int32),
            pltpu.SMEM((2, capacity, batch_rows, table_width), jnp.int32),
            dma((planes + 1,)),
            dma((planes + 3,)),
            dma((7 + key_heads * per_group,)),
            dma((planes, sources)),
            dma((planes, sources)),
            dma((group_count,)),
            dma((group_count,)),
            dma((sources,)),
            dma((sources,)),
            dma((sources,)),
            dma((sources,)),
            dma((sources,)),
            dma((sources,)),
            pltpu.SemaphoreType.REGULAR((tp_count,)),
            pltpu.SemaphoreType.REGULAR((tp_count,)),
            dma((sources,)),
            dma((sources,)),
            dma((tp_count,)),
            dma((tp_count,)),
        ],
        compiler_params=pltpu.CompilerParams(
            collective_id=0, has_side_effects=True, vmem_limit_bytes=40 * 2**20
        ),
    )(
        *(
            pltpu.with_memory_space_constraint(operand, pltpu.HBM)
            for operand in (
                lengths,
                block_table,
                block_scale.reshape(pool_slots, planes).T,
                queries,
                cache_pool.reshape(pool_slots, planes, block_size, head_size),
                output_weight,
            )
        )
    )
    decode_cache, decode_scale, output = pl.pallas_call(
        copy_out_kernel,
        out_shape=(
            jax.ShapeDtypeStruct((positions, planes, block_size, head_size), bf16),
            jax.ShapeDtypeStruct(results[3].shape, bf16),
            jax.ShapeDtypeStruct(results[4].shape, bf16),
        ),
        in_specs=[vmem] * 5,
        out_specs=(hbm,) * 3,
        scratch_shapes=[
            pltpu.SMEM((batch_rows, table_width), jnp.int32),
            dma((11,)),
            dma,
        ],
        compiler_params=pltpu.CompilerParams(vmem_limit_bytes=16 * 2**20),
    )(*(pltpu.with_memory_space_constraint(r, pltpu.VMEM) for r in results))
    return (
        output,
        decode_cache.reshape(per_group, share_blocks, key_heads, 2, block_size, head_size),
        decode_scale.transpose(0, 2, 1).reshape(per_group, share_blocks, key_heads, 2),
    )


def solution(mesh):
    placed = (
        P("grp", "tp", None),
        P(("seq", "grp"), "tp", None, None, None),
        P(("seq", "grp"), "tp", None),
        P(),
        P(),
        P("tp", ("seq", "grp")),
    )
    return jax.shard_map(
        per_device,
        mesh=mesh,
        in_specs=placed,
        out_specs=(
            P("tp", ("seq", "grp")),
            P("grp", "seq", "tp", None, None, None),
            P("grp", "seq", "tp", None),
        ),
        check_vma=False,
    )
```

```python
import functools
import math

import jax
import jax.numpy as jnp
from jax import lax
from jax.experimental import pallas as pl
from jax.experimental.pallas import tpu as pltpu
from jax.sharding import PartitionSpec as P

MESH = pl.DeviceIdType.MESH
absent_score = -1e30
absent_limit = -1e29


def xor_index(index, mask):
    out = index
    bit = 1
    while bit <= mask:
        if mask & bit:
            out = out + bit - 2 * bit * ((index // bit) % 2)
        bit *= 2
    return out


def exchange_kernel(
    dims,
    lengths_in,
    table_in,
    block_scale_in,
    queries_in,
    pool_ref,
    weight_ref,
    placed_ref,
    last_ref,
    arrival_rows,
    scales_out_ref,
    output_ref,
    lengths_ref,
    table_ref,
    block_scale_ref,
    queries_ref,
    raw,
    send,
    arrived,
    weights,
    all_queries,
    scores,
    peaks,
    sums,
    accums,
    parts,
    parts_in,
    stats,
    stats_in,
    attended,
    projected,
    projected_in,
    scales_in,
    scales_wide,
    pick_rows,
    scale_words,
    arrival_words,
    pick_words,
    load_sems,
    local_sems,
    word_sems,
    block_send,
    block_recv,
    tail_blocks,
    tail_sems,
    query_send,
    query_recv,
    scale_send,
    scale_recv,
    part_send,
    part_recv,
    stat_send,
    stat_recv,
    known_below,
    known_above,
    att_send,
    att_recv,
    proj_send,
    proj_recv,
):
    seq_count, group_count, tp_count, per_group, root_scale = dims
    sources = seq_count * group_count
    seq_index = lax.axis_index("seq")
    group_index = lax.axis_index("grp")
    tp_index = lax.axis_index("tp")
    me = seq_index * group_count + group_index
    planes, _, capacity, block_size, head_size = send.shape
    arrived = [*arrived, last_ref]
    pool_slots = raw[0].shape[0]
    key_heads = planes // 2
    query_rows = all_queries.shape[2]
    groups = query_rows // per_group
    batch_rows, table_width = table_ref.shape
    share_blocks = table_width // seq_count
    positions = per_group * share_blocks
    row_share = parts.shape[1]
    per_tile = groups // row_share
    f32, bf16 = jnp.float32, jnp.bfloat16

    def pool_load(plane):
        return pltpu.make_async_copy(pool_ref.at[:, plane], raw[plane], load_sems.at[plane])

    table_load = pltpu.make_async_copy(table_in, table_ref, word_sems.at[4])
    small_loads = [
        pltpu.make_async_copy(lengths_in, lengths_ref, word_sems.at[5]),
        pltpu.make_async_copy(block_scale_in, block_scale_ref, word_sems.at[6]),
    ] + [
        pltpu.make_async_copy(
            queries_in.at[request, pl.ds(head * groups, groups)],
            queries_ref.at[head, pl.ds(request * groups, groups)],
            word_sems.at[7 + head * per_group + request],
        )
        for head in range(key_heads)
        for request in range(per_group)
    ]
    table_load.start()
    pool_load(0).start()

    def source_device(other):
        return {"seq": other // group_count, "grp": other % group_count}

    barrier = pltpu.get_barrier_semaphore()
    for step in range(1, sources):
        pl.semaphore_signal(
            barrier, inc=1, device_id=source_device(xor_index(me, step)), device_id_type=MESH
        )
    below, above = tp_index > 0, tp_index < tp_count - 1

    @pl.when(above)
    def _():
        pl.semaphore_signal(
            barrier, inc=1, device_id={"tp": tp_index + 1}, device_id_type=MESH
        )

    wide = (batch_rows, table_width)
    table_load.wait()
    table = table_ref[...]
    row_of = lax.broadcasted_iota(jnp.int32, wide, 0)
    col_of = lax.broadcasted_iota(jnp.int32, wide, 1)
    square = (table_width, table_width)
    upper = lax.broadcasted_iota(jnp.int32, square, 0)
    lower = lax.broadcasted_iota(jnp.int32, square, 1)
    alike = upper // share_blocks == lower // share_blocks
    all_alike = jnp.where(alike, 1.0, 0.0).astype(bf16)
    earlier = jnp.where(alike, jnp.where(upper < lower, 1.0, 0.0), 0.0).astype(bf16)
    owner = table // pool_slots
    local = (table % pool_slots).astype(f32)

    def ranks(theirs):
        ones = jnp.where(theirs, 1.0, 0.0).astype(bf16)
        rank = jnp.dot(ones, earlier, preferred_element_type=f32)
        whole = jnp.dot(ones, all_alike, preferred_element_type=f32)
        for request in range(batch_rows):
            last = request // per_group * per_group + per_group
            for later in range(request + 1, last):
                rank = rank + jnp.where(row_of == later, whole[request : request + 1], 0.0)
        return rank

    range_of = jnp.where(upper // share_blocks == lower, 1.0, 0.0).astype(bf16)
    own_rank = jnp.where(owner == me, ranks(owner == me), -1.0)

    def pick(kind, values):
        for within in range(capacity):
            pick_rows[kind, within] = jnp.dot(
                jnp.where(own_rank == within, values, 0.0).astype(bf16),
                range_of,
                preferred_element_type=f32,
            ).astype(jnp.int32)
        return pltpu.make_async_copy(
            pick_rows.at[kind], pick_words.at[kind], word_sems.at[kind]
        )

    slot_copy = pick(0, local)
    slot_copy.start()
    own_queries = pltpu.make_async_copy(queries_ref, all_queries.at[group_index], local_sems.at[0])
    pl.semaphore_wait(barrier, sources - 1 + jnp.where(below, 1, 0))

    def query_copy(step):
        return pltpu.make_async_remote_copy(
            src_ref=queries_ref,
            dst_ref=all_queries.at[group_index],
            send_sem=query_send.at[step],
            recv_sem=query_recv.at[step],
            device_id={"grp": xor_index(group_index, step)},
            device_id_type=MESH,
        )

    def scale_copy(step):
        return pltpu.make_async_remote_copy(
            src_ref=block_scale_ref,
            dst_ref=scales_in.at[me],
            send_sem=scale_send.at[step],
            recv_sem=scale_recv.at[step],
            device_id=source_device(xor_index(me, step)),
            device_id_type=MESH,
        )

    own_scales = pltpu.make_async_copy(block_scale_ref, scales_in.at[me], local_sems.at[1])

    def block_copy(plane, step):
        other = xor_index(me, step)
        return pltpu.make_async_remote_copy(
            src_ref=send.at[plane, other],
            dst_ref=arrived[plane].at[pl.ds(me * capacity, capacity)],
            send_sem=block_send.at[plane, step],
            recv_sem=block_recv.at[plane, step],
            device_id=source_device(other),
            device_id_type=MESH,
        )

    def own_blocks(plane):
        return pltpu.make_async_copy(
            send.at[plane, me],
            arrived[plane].at[pl.ds(me * capacity, capacity)],
            local_sems.at[2 + plane],
        )

    steps = sorted(range(1, sources), key=lambda s: (s // group_count == 0, s % group_count, s))
    near_steps = [s for s in steps if (s // group_count).bit_count() <= 1]
    far_steps = [s for s in steps if s not in near_steps]

    tail_plane, tail_step = planes - 1, far_steps[-1] if far_steps else 0
    kept = capacity - tail_blocks.shape[0]
    origin = (seq_count - 1) * group_count
    to_relay = group_count * (1 << max(tail_step // group_count, 1).bit_length() - 1)
    to_relay += tail_step % group_count
    hands_over = me == origin
    relays = me == origin ^ to_relay

    def far_copy(plane, step):
        if (plane, step) != (tail_plane, tail_step):
            return block_copy(plane, step)
        other = xor_index(me, step)
        return pltpu.make_async_remote_copy(
            src_ref=send.at[plane, other, pl.ds(0, kept)],
            dst_ref=arrived[plane].at[pl.ds(me * capacity, kept)],
            send_sem=block_send.at[plane, step],
            recv_sem=block_recv.at[plane, step],
            device_id=source_device(other),
            device_id_type=MESH,
        )

    def tail_copy(source, owner, route, sent, received):
        return pltpu.make_async_remote_copy(
            src_ref=source,
            dst_ref=arrived[tail_plane].at[
                pl.ds(owner * capacity + kept, capacity - kept)
            ],
            send_sem=sent,
            recv_sem=received,
            device_id=source_device(xor_index(me, route)),
            device_id_type=MESH,
        )

    if far_steps:
        tail_source = send.at[tail_plane, xor_index(me, tail_step), pl.ds(kept, capacity - kept)]
        tail_direct = tail_copy(
            tail_source, me, tail_step, tail_sems.at[0], tail_sems.at[1]
        )
        tail_passed = tail_copy(
            tail_blocks,
            xor_index(me, to_relay),
            tail_step ^ to_relay,
            tail_sems.at[2],
            tail_sems.at[1],
        )
        tail_handed = pltpu.make_async_remote_copy(
            src_ref=tail_source,
            dst_ref=tail_blocks,
            send_sem=tail_sems.at[3],
            recv_sem=tail_sems.at[4],
            device_id=source_device(xor_index(me, to_relay)),
            device_id_type=MESH,
        )

    def picked(kind, other, within, request):
        group = other % group_count
        return pick_words[kind, within, group * per_group + request, other // group_count]

    def slot_of(other, within):
        slot = picked(0, other, within, 0)
        for request in range(1, per_group):
            slot = slot + picked(0, other, within, request)
        return jnp.clip(slot, 0, pool_slots - 1)

    def sort_blocks(plane, other):
        def place(within, _):
            send[plane, other, within] = raw[plane][slot_of(other, within)]
            return 0

        lax.fori_loop(0, capacity, place, 0)

    def sort_plane(plane):
        def place(other, _):
            sort_blocks(plane, other)
            return 0

        lax.fori_loop(0, sources, place, 0)

    def send_plane(plane, chosen):
        for step in chosen:
            block_copy(plane, step).start()

    slot_copy.wait()
    pool_load(0).wait()
    for place, step in enumerate(near_steps):
        other = xor_index(me, step)
        for within in range(capacity):
            send[0, other, within] = raw[0][slot_of(other, within)]
        if place:
            block_copy(0, near_steps[place - 1]).start()
    sort_blocks(0, me)
    block_copy(0, near_steps[-1]).start()
    for copy in small_loads:
        copy.start()
    for plane in range(1, planes):
        pool_load(plane).start()
    for copy in small_loads:
        copy.wait()
    own_queries.start()
    for step in range(1, group_count):
        query_copy(step).start()
    for step in steps:
        scale_copy(step).start()
    own_scales.start()
    weight_load = pltpu.make_async_copy(weight_ref, weights, load_sems.at[planes])
    weight_load.start()
    for step in far_steps:
        sort_blocks(0, xor_index(me, step))
    for plane in range(1, planes):
        pool_load(plane).wait()
        sort_plane(plane)
        if plane == 1:
            send_plane(plane, near_steps)
    if far_steps:
        pl.when(hands_over)(tail_handed.start)
    for plane in range(planes):
        own_blocks(plane).start()

    arrival = jnp.zeros(wide, f32)
    for source in range(sources):
        theirs = owner == source
        arrival = jnp.where(theirs, ranks(theirs) + source * capacity, arrival)
    arrival_rows[...] = arrival.astype(jnp.int32)
    context = jnp.full(wide, lengths_ref[0], jnp.int32)
    for request in range(1, batch_rows):
        context = jnp.where(row_of == request, lengths_ref[request], context)
    live = jnp.clip(context - col_of * block_size, 0, block_size).astype(f32)
    scales_wide[...] = block_scale_ref[...].astype(f32)
    word_copies = [
        pick(1, live),
        pltpu.make_async_copy(arrival_rows, arrival_words, word_sems.at[2]),
        pltpu.make_async_copy(scales_wide, scale_words, word_sems.at[3]),
    ]
    for copy in word_copies:
        copy.start()
    for copy in word_copies:
        copy.wait()

    own_queries.wait()
    for step in range(1, group_count):
        query_copy(step).wait()

    lanes = lax.broadcasted_iota(jnp.int32, (query_rows, block_size), 1)
    row_ids = lax.broadcasted_iota(jnp.int32, (query_rows, block_size), 0)
    share_lanes = lax.broadcasted_iota(jnp.int32, (row_share, head_size), 1)
    share_rows = lax.broadcasted_iota(jnp.int32, (row_share, head_size), 0)
    for head in range(key_heads):
        peaks[...] = jnp.full_like(peaks, absent_score)
        sums[...] = jnp.zeros_like(sums)
        accums[...] = jnp.zeros_like(accums)

        def score_blocks(other, _):
            group = other % group_count
            keys = send[2 * head, other].reshape(capacity * block_size, head_size)
            raw_scores = lax.dot_general(
                all_queries[group, head],
                keys,
                (((1,), (1,)), ((), ())),
                preferred_element_type=jnp.float32,
            )
            highest = peaks[group]
            for within in range(capacity):
                limit = jnp.full(lanes.shape, picked(1, other, within, 0), jnp.int32)
                for request in range(1, per_group):
                    limit = jnp.where(
                        row_ids >= request * groups, picked(1, other, within, request), limit
                    )
                part = raw_scores[:, within * block_size : (within + 1) * block_size]
                part = part * scale_words[2 * head, slot_of(other, within)] * root_scale
                part = jnp.where(lanes < limit, part, absent_score)
                scores[other, :, within * block_size : (within + 1) * block_size] = part
                highest = jnp.maximum(highest, part)
            peaks[group] = highest
            return 0

        lax.fori_loop(0, sources, score_blocks, 0)
        for group in range(group_count):
            peaks[group] = jnp.broadcast_to(
                jnp.max(peaks[group], axis=1, keepdims=True), lanes.shape
            )

        def weigh_blocks(other, _):
            group = other % group_count
            peak = peaks[group]
            total = sums[group]
            pieces = []
            for within in range(capacity):
                part = scores[other, :, within * block_size : (within + 1) * block_size]
                weight = jnp.where(part > absent_limit, jnp.exp(part - peak), 0.0)
                total = total + weight
                pieces.append(
                    (weight * scale_words[2 * head + 1, slot_of(other, within)]).astype(bf16)
                )
            sums[group] = total
            values = send[2 * head + 1, other].reshape(capacity * block_size, head_size)
            accums[group] += jnp.dot(
                jnp.concatenate(pieces, axis=1), values, preferred_element_type=jnp.float32
            )
            return 0

        lax.fori_loop(0, sources, weigh_blocks, 0)
        for group in range(group_count):
            total = jnp.broadcast_to(jnp.sum(sums[group], axis=1, keepdims=True), lanes.shape)
            for request in range(per_group):
                tile = (group * key_heads + head) * per_group + request
                for piece in range(per_tile):
                    low = request * groups + piece * row_share
                    place = tile * per_tile + piece
                    parts[place] = accums[group, low : low + row_share].astype(bf16)
                    stats[place] = jnp.sum(
                        jnp.where(
                            share_lanes == share_rows, peaks[group, low : low + row_share], 0.0
                        )
                        + jnp.where(
                            share_lanes == share_rows + row_share,
                            total[low : low + row_share],
                            0.0,
                        ),
                        axis=0,
                        keepdims=True,
                    )

    def part_copy(step):
        other = xor_index(me, step)
        return pltpu.make_async_remote_copy(
            src_ref=parts.at[other],
            dst_ref=parts_in.at[me],
            send_sem=part_send.at[step],
            recv_sem=part_recv.at[step],
            device_id=source_device(other),
            device_id_type=MESH,
        )

    def stat_copy(step):
        other = xor_index(me, step)
        return pltpu.make_async_remote_copy(
            src_ref=stats.at[other],
            dst_ref=stats_in.at[me],
            send_sem=stat_send.at[step],
            recv_sem=stat_recv.at[step],
            device_id=source_device(other),
            device_id_type=MESH,
        )

    for step in steps:
        stat_copy(step).start()
        part_copy(step).start()
    parts_in[me] = parts[me]
    stats_in[me] = stats[me]
    for plane in range(2, min(planes, 3)):
        send_plane(plane, near_steps)

    @pl.when(below)
    def _():
        pl.semaphore_signal(
            known_above.at[0], inc=1, device_id={"tp": tp_index - 1}, device_id_type=MESH
        )

    @pl.when(above)
    def _():
        pl.semaphore_wait(known_above.at[0], 1)

    for reach in range(1, tp_count - 1):

        @pl.when(jnp.logical_and(tp_index >= reach, above))
        def _():
            pl.semaphore_signal(
                known_below.at[reach], inc=1, device_id={"tp": tp_index + 1}, device_id_type=MESH
            )

        @pl.when(jnp.logical_and(tp_index + reach < tp_count, below))
        def _():
            pl.semaphore_signal(
                known_above.at[reach], inc=1, device_id={"tp": tp_index - 1}, device_id_type=MESH
            )

        @pl.when(tp_index - 1 >= reach)
        def _():
            pl.semaphore_wait(known_below.at[reach], 1)

        @pl.when(tp_index + 1 + reach < tp_count)
        def _():
            pl.semaphore_wait(known_above.at[reach], 1)

    for step in steps:
        stat_copy(step).wait_recv()
        part_copy(step).wait_recv()

    def spread(source, first):
        return jnp.broadcast_to(
            jnp.sum(
                jnp.where(
                    share_lanes == share_rows + first,
                    jnp.broadcast_to(stats_in[source], share_lanes.shape),
                    0.0,
                ),
                axis=1,
                keepdims=True,
            ),
            share_lanes.shape,
        )

    source_peaks = [spread(source, 0) for source in range(sources)]
    highest = functools.reduce(jnp.maximum, source_peaks)
    numerator = jnp.zeros_like(highest)
    denominator = jnp.zeros_like(highest)
    for source in range(sources):
        factor = jnp.exp(source_peaks[source] - highest)
        numerator += parts_in[source].astype(f32) * factor
        denominator += spread(source, row_share) * factor
    attended[me] = (numerator / denominator).astype(jnp.bfloat16)

    def att_copy(step):
        return pltpu.make_async_remote_copy(
            src_ref=attended.at[me],
            dst_ref=attended.at[me],
            send_sem=att_send.at[step],
            recv_sem=att_recv.at[step],
            device_id=source_device(xor_index(me, step)),
            device_id_type=MESH,
        )

    weight_load.wait()
    for step in steps:
        att_copy(step).start()
    for plane in range(3, planes):
        send_plane(plane, near_steps)
    for step in steps:
        att_copy(step).wait_recv()
    for plane in range(planes):
        for step in near_steps:
            if step // group_count == 1:
                block_copy(plane, step).wait_send()
    if far_steps:

        @pl.when(relays)
        def _():
            tail_handed.wait_recv()
            tail_passed.start()

    for plane in range(planes):
        for step in far_steps:
            far_copy(plane, step).start()
    if far_steps:
        pl.when(jnp.logical_not(hands_over))(tail_direct.start)

    rows = sources * row_share
    gathered = attended[...].astype(f32).reshape(rows, head_size)
    row = lax.broadcasted_iota(jnp.int32, (rows, head_size), 0)
    row_head = (row // (groups * per_group)) % key_heads * groups + row % groups
    left = jnp.concatenate(
        [
            jnp.where(row_head == head, gathered, 0.0).astype(jnp.bfloat16)
            for head in range(key_heads * groups)
        ],
        axis=1,
    )
    columns = weights.shape[1]
    width = min(columns, 256)
    here = batch_rows // tp_count
    for low in range(0, columns, width):
        product = jnp.dot(left, weights[:, low : low + width], preferred_element_type=jnp.float32)
        for request in range(batch_rows):
            group, inner = request // per_group, request % per_group
            total = jnp.zeros((1, width), jnp.float32)
            for head in range(key_heads):
                tile = (group * key_heads + head) * per_group + inner
                total += jnp.sum(
                    product[tile * groups : (tile + 1) * groups], axis=0, keepdims=True
                )
            projected[request // here, pl.ds(request % here, 1), low : low + width] = total

    def proj_copy(step):
        other = xor_index(tp_index, step)
        return pltpu.make_async_remote_copy(
            src_ref=projected.at[other],
            dst_ref=projected_in.at[tp_index],
            send_sem=proj_send.at[step],
            recv_sem=proj_recv.at[step],
            device_id={"tp": other},
            device_id_type=MESH,
        )

    for step in range(1, tp_count):
        proj_copy(step).start()
    projected_in[tp_index] = projected[tp_index]
    for step in range(1, tp_count):
        proj_copy(step).wait()
    total = projected_in[0]
    for source in range(1, tp_count):
        total += projected_in[source]
    output_ref[...] = total.astype(output_ref.dtype)

    own_scales.wait()
    for step in steps:
        scale_copy(step).wait()
    slot_ids = lax.broadcasted_iota(jnp.int32, (pool_slots, table_width), 0)
    wanted = jnp.where(
        lax.broadcasted_iota(jnp.int32, (table_width, share_blocks), 0)
        == lax.broadcasted_iota(jnp.int32, (table_width, share_blocks), 1)
        + seq_index * share_blocks,
        1.0,
        0.0,
    ).astype(bf16)
    for request in range(per_group):
        slots = table_ref[pl.ds(group_index * per_group + request, 1), :]
        found = jnp.zeros((planes, table_width), f32)
        for source in range(sources):
            onehot = jnp.where(slots == slot_ids + source * pool_slots, 1.0, 0.0).astype(bf16)
            found += jnp.dot(scales_in[source], onehot, preferred_element_type=f32)
        scales_out_ref[request] = jnp.dot(
            found.astype(bf16), wanted, preferred_element_type=f32
        ).astype(bf16)

    unroll = 4 if share_blocks % 4 == 0 else 1
    for plane in range(planes - 1):
        own_blocks(plane).wait()
        for step in steps:
            (block_copy if step in near_steps else far_copy)(plane, step).wait_recv()
        for request in range(per_group):

            def place(turn, _):
                for part in range(unroll):
                    column = turn * unroll + part
                    index = arrival_words[
                        group_index * per_group + request, seq_index * share_blocks + column
                    ]
                    placed_ref[request * share_blocks + column, plane] = arrived[plane][
                        jnp.clip(index, 0, positions - 1)
                    ]
                return 0

            lax.fori_loop(0, share_blocks // unroll, place, 0)
    for step in steps:
        part_copy(step).wait_send()
        stat_copy(step).wait_send()
        att_copy(step).wait_send()
    own_blocks(planes - 1).wait()
    for step in near_steps:
        block_copy(planes - 1, step).wait_recv()
    for plane in range(planes):
        for step in far_steps:
            far_copy(plane, step).wait_send()
    for plane in range(planes):
        for step in near_steps:
            if step // group_count != 1:
                block_copy(plane, step).wait_send()
    if far_steps:
        pl.when(hands_over)(tail_handed.wait_send)
        pl.when(relays)(tail_passed.wait_send)
        pl.when(jnp.logical_not(hands_over))(tail_direct.wait_send)
    for step in far_steps:
        far_copy(planes - 1, step).wait_recv()
    if far_steps:
        tail_direct.wait_recv()


def copy_out_kernel(
    placed_in,
    last_in,
    arrival_in,
    scale_in,
    output_in,
    cache_ref,
    scale_ref,
    output_ref,
    arrival_words,
    sems,
    block_sem,
):
    positions, first = placed_in.shape[:2]
    per_group, _, share_blocks = scale_in.shape
    group_index, seq_index = lax.axis_index("grp"), lax.axis_index("seq")
    words = pltpu.make_async_copy(arrival_in, arrival_words, sems.at[0])
    words.start()
    chunks = 8
    share = positions // chunks
    copies = [
        pltpu.make_async_copy(
            placed_in.at[pl.ds(part * share, share)],
            cache_ref.at[pl.ds(part * share, share), pl.ds(0, first)],
            sems.at[3 + part],
        )
        for part in range(chunks)
    ]
    copies.append(pltpu.make_async_copy(scale_in, scale_ref, sems.at[1]))
    copies.append(pltpu.make_async_copy(output_in, output_ref, sems.at[2]))
    for copy in copies:
        copy.start()
    words.wait()

    def block(position):
        index = arrival_words[
            group_index * per_group + position // share_blocks,
            seq_index * share_blocks + position % share_blocks,
        ]
        return pltpu.make_async_copy(
            last_in.at[jnp.clip(index, 0, positions - 1)],
            cache_ref.at[position, first],
            block_sem,
        )

    def start(position, _):
        block(position).start()
        return 0

    lax.fori_loop(0, positions, start, 0, unroll=4)
    for copy in copies:
        copy.wait()
    pltpu.make_async_copy(last_in, cache_ref.at[:, first], block_sem).wait()


def per_device(queries, cache_pool, block_scale, block_table, lengths, output_weight):
    seq_count = lax.axis_size("seq")
    group_count = lax.axis_size("grp")
    tp_count = lax.axis_size("tp")
    sources = seq_count * group_count
    pool_slots, key_heads, _, block_size, head_size = cache_pool.shape
    batch_rows, table_width = block_table.shape
    per_group = batch_rows // group_count
    share_blocks = table_width // seq_count
    capacity = pool_slots // sources
    heads_here = queries.shape[1]
    groups = heads_here // key_heads
    planes = key_heads * 2
    positions = per_group * share_blocks
    columns = output_weight.shape[1]
    root_scale = 1.0 / math.sqrt(head_size)

    row_share = batch_rows * key_heads * groups // sources
    query_rows = per_group * groups
    f32, bf16 = jnp.float32, jnp.bfloat16
    dma = pltpu.SemaphoreType.DMA
    vmem = pl.BlockSpec(memory_space=pltpu.VMEM)
    hbm = pl.BlockSpec(memory_space=pltpu.HBM)
    here = batch_rows // tp_count
    results = pl.pallas_call(
        functools.partial(
            exchange_kernel, (seq_count, group_count, tp_count, per_group, root_scale)
        ),
        out_shape=(
            pltpu.VMEM((positions, planes - 1, block_size, head_size), bf16),
            pltpu.VMEM((positions, block_size, head_size), bf16),
            pltpu.VMEM((batch_rows, table_width), jnp.int32),
            pltpu.VMEM((per_group, planes, share_blocks), bf16),
            pltpu.VMEM((here, columns), bf16),
        ),
        in_specs=[hbm, hbm, hbm, hbm, hbm, hbm],
        out_specs=(vmem,) * 5,
        scratch_shapes=[
            pltpu.SMEM((batch_rows,), jnp.int32),
            pltpu.VMEM((batch_rows, table_width), jnp.int32),
            pltpu.VMEM((planes, pool_slots), bf16),
            pltpu.VMEM((key_heads, query_rows, head_size), bf16),
            [pltpu.VMEM((pool_slots, block_size, head_size), bf16) for _ in range(planes)],
            pltpu.VMEM((planes, sources, capacity, block_size, head_size), bf16),
            [pltpu.VMEM((pool_slots, block_size, head_size), bf16) for _ in range(planes - 1)],
            pltpu.VMEM((heads_here * head_size, columns), bf16),
            pltpu.VMEM((group_count, key_heads, query_rows, head_size), bf16),
            pltpu.VMEM((sources, query_rows, capacity * block_size), f32),
            pltpu.VMEM((group_count, query_rows, block_size), f32),
            pltpu.VMEM((group_count, query_rows, block_size), f32),
            pltpu.VMEM((group_count, query_rows, head_size), f32),
            pltpu.VMEM((sources, row_share, head_size), bf16),
            pltpu.VMEM((sources, row_share, head_size), bf16),
            pltpu.VMEM((sources, 1, head_size), f32),
            pltpu.VMEM((sources, 1, head_size), f32),
            pltpu.VMEM((sources, row_share, head_size), bf16),
            pltpu.VMEM((tp_count, here, columns), f32),
            pltpu.VMEM((tp_count, here, columns), f32),
            pltpu.VMEM((sources, planes, pool_slots), bf16),
            pltpu.VMEM((planes, pool_slots), f32),
            pltpu.VMEM((2, capacity, batch_rows, table_width), jnp.int32),
            pltpu.SMEM((planes, pool_slots), f32),
            pltpu.SMEM((batch_rows, table_width), jnp.int32),
            pltpu.SMEM((2, capacity, batch_rows, table_width), jnp.int32),
            dma((planes + 1,)),
            dma((planes + 3,)),
            dma((7 + key_heads * per_group,)),
            dma((planes, sources)),
            dma((planes, sources)),
            pltpu.VMEM((max(capacity // 4, 1), block_size, head_size), bf16),
            dma((5,)),
            dma((group_count,)),
            dma((group_count,)),
            dma((sources,)),
            dma((sources,)),
            dma((sources,)),
            dma((sources,)),
            dma((sources,)),
            dma((sources,)),
            pltpu.SemaphoreType.REGULAR((tp_count,)),
            pltpu.SemaphoreType.REGULAR((tp_count,)),
            dma((sources,)),
            dma((sources,)),
            dma((tp_count,)),
            dma((tp_count,)),
        ],
        compiler_params=pltpu.CompilerParams(
            collective_id=0, has_side_effects=True, vmem_limit_bytes=40 * 2**20
        ),
    )(
        *(
            pltpu.with_memory_space_constraint(operand, pltpu.HBM)
            for operand in (
                lengths,
                block_table,
                block_scale.reshape(pool_slots, planes).T,
                queries,
                cache_pool.reshape(pool_slots, planes, block_size, head_size),
                output_weight,
            )
        )
    )
    decode_cache, decode_scale, output = pl.pallas_call(
        copy_out_kernel,
        out_shape=(
            jax.ShapeDtypeStruct((positions, planes, block_size, head_size), bf16),
            jax.ShapeDtypeStruct(results[3].shape, bf16),
            jax.ShapeDtypeStruct(results[4].shape, bf16),
        ),
        in_specs=[vmem] * 5,
        out_specs=(hbm,) * 3,
        scratch_shapes=[
            pltpu.SMEM((batch_rows, table_width), jnp.int32),
            dma((11,)),
            dma,
        ],
        compiler_params=pltpu.CompilerParams(vmem_limit_bytes=16 * 2**20),
    )(*(pltpu.with_memory_space_constraint(r, pltpu.VMEM) for r in results))
    return (
        output,
        decode_cache.reshape(per_group, share_blocks, key_heads, 2, block_size, head_size),
        decode_scale.transpose(0, 2, 1).reshape(per_group, share_blocks, key_heads, 2),
    )


def solution(mesh):
    placed = (
        P("grp", "tp", None),
        P(("seq", "grp"), "tp", None, None, None),
        P(("seq", "grp"), "tp", None),
        P(),
        P(),
        P("tp", ("seq", "grp")),
    )
    return jax.shard_map(
        per_device,
        mesh=mesh,
        in_specs=placed,
        out_specs=(
            P("tp", ("seq", "grp")),
            P("grp", "seq", "tp", None, None, None),
            P("grp", "seq", "tp", None),
        ),
        check_vma=False,
    )
```

```python
import functools
import math

import jax
import jax.numpy as jnp
from jax import lax
from jax.experimental import pallas as pl
from jax.experimental.pallas import tpu as pltpu
from jax.sharding import PartitionSpec as P

MESH = pl.DeviceIdType.MESH
absent_score = -1e30
absent_limit = -1e29


def xor_index(index, mask):
    out = index
    bit = 1
    while bit <= mask:
        if mask & bit:
            out = out + bit - 2 * bit * ((index // bit) % 2)
        bit *= 2
    return out


def exchange_kernel(
    dims,
    lengths_in,
    table_in,
    block_scale_in,
    queries_in,
    pool_ref,
    weight_ref,
    placed_ref,
    last_ref,
    arrival_rows,
    scales_out_ref,
    output_ref,
    lengths_ref,
    table_ref,
    block_scale_ref,
    queries_ref,
    raw,
    send,
    arrived,
    weights,
    all_queries,
    scores,
    peaks,
    sums,
    accums,
    parts,
    parts_in,
    stats,
    stats_in,
    attended,
    projected,
    projected_in,
    scales_in,
    scales_wide,
    pick_rows,
    scale_words,
    arrival_words,
    pick_words,
    slot_rows,
    slot_words,
    load_sems,
    local_sems,
    word_sems,
    block_send,
    block_recv,
    tail_blocks,
    tail_sems,
    query_send,
    query_recv,
    scale_send,
    scale_recv,
    part_send,
    part_recv,
    stat_send,
    stat_recv,
    known_below,
    known_above,
    att_send,
    att_recv,
    proj_send,
    proj_recv,
):
    seq_count, group_count, tp_count, per_group, root_scale = dims
    sources = seq_count * group_count
    seq_index = lax.axis_index("seq")
    group_index = lax.axis_index("grp")
    tp_index = lax.axis_index("tp")
    me = seq_index * group_count + group_index
    planes, _, capacity, block_size, head_size = send.shape
    arrived = [*arrived, last_ref]
    pool_slots = raw[0].shape[0]
    key_heads = planes // 2
    query_rows = all_queries.shape[2]
    groups = query_rows // per_group
    batch_rows, table_width = table_ref.shape
    share_blocks = table_width // seq_count
    positions = per_group * share_blocks
    row_share = parts.shape[1]
    per_tile = groups // row_share
    f32, bf16 = jnp.float32, jnp.bfloat16

    def pool_load(plane):
        return pltpu.make_async_copy(pool_ref.at[:, plane], raw[plane], load_sems.at[plane])

    table_load = pltpu.make_async_copy(table_in, table_ref, word_sems.at[4])
    small_loads = [
        pltpu.make_async_copy(lengths_in, lengths_ref, word_sems.at[5]),
        pltpu.make_async_copy(block_scale_in, block_scale_ref, word_sems.at[6]),
    ] + [
        pltpu.make_async_copy(
            queries_in.at[request, pl.ds(head * groups, groups)],
            queries_ref.at[head, pl.ds(request * groups, groups)],
            word_sems.at[7 + head * per_group + request],
        )
        for head in range(key_heads)
        for request in range(per_group)
    ]
    table_load.start()
    pool_load(0).start()

    def source_device(other):
        return {"seq": other // group_count, "grp": other % group_count}

    barrier = pltpu.get_barrier_semaphore()
    for step in range(1, sources):
        pl.semaphore_signal(
            barrier, inc=1, device_id=source_device(xor_index(me, step)), device_id_type=MESH
        )
    below, above = tp_index > 0, tp_index < tp_count - 1

    @pl.when(above)
    def _():
        pl.semaphore_signal(
            barrier, inc=1, device_id={"tp": tp_index + 1}, device_id_type=MESH
        )

    wide = (batch_rows, table_width)
    table_load.wait()
    table = table_ref[...]
    row_of = lax.broadcasted_iota(jnp.int32, wide, 0)
    col_of = lax.broadcasted_iota(jnp.int32, wide, 1)
    square = (table_width, table_width)
    upper = lax.broadcasted_iota(jnp.int32, square, 0)
    lower = lax.broadcasted_iota(jnp.int32, square, 1)
    alike = upper // share_blocks == lower // share_blocks
    all_alike = jnp.where(alike, 1.0, 0.0).astype(bf16)
    earlier = jnp.where(alike, jnp.where(upper < lower, 1.0, 0.0), 0.0).astype(bf16)
    owner = table // pool_slots
    local = (table % pool_slots).astype(f32)

    def ranks(theirs):
        ones = jnp.where(theirs, 1.0, 0.0).astype(bf16)
        rank = jnp.dot(ones, earlier, preferred_element_type=f32)
        whole = jnp.dot(ones, all_alike, preferred_element_type=f32)
        for request in range(batch_rows):
            last = request // per_group * per_group + per_group
            for later in range(request + 1, last):
                rank = rank + jnp.where(row_of == later, whole[request : request + 1], 0.0)
        return rank

    range_of = jnp.where(upper // share_blocks == lower, 1.0, 0.0).astype(bf16)
    own_rank = jnp.where(owner == me, ranks(owner == me), -1.0)

    rank_rows = lax.broadcasted_iota(jnp.int32, (capacity, table_width), 0).astype(f32)
    slots = jnp.zeros((capacity, table_width), f32)
    for request in range(batch_rows):
        column = upper // share_blocks + request // per_group * seq_count
        slots += jnp.dot(
            jnp.where(
                own_rank[request : request + 1] == rank_rows, local[request : request + 1], 0.0
            ).astype(bf16),
            jnp.where(column == lower, 1.0, 0.0).astype(bf16),
            preferred_element_type=f32,
        )
    slot_rows[...] = slots.astype(jnp.int32)
    slot_copy = pltpu.make_async_copy(slot_rows, slot_words, word_sems.at[0])
    slot_copy.start()

    def pick(values):
        for within in range(capacity):
            pick_rows[within] = jnp.dot(
                jnp.where(own_rank == within, values, 0.0).astype(bf16),
                range_of,
                preferred_element_type=f32,
            ).astype(jnp.int32)
        return pltpu.make_async_copy(pick_rows, pick_words, word_sems.at[1])

    own_queries = pltpu.make_async_copy(queries_ref, all_queries.at[group_index], local_sems.at[0])
    pl.semaphore_wait(barrier, sources - 1 + jnp.where(below, 1, 0))

    def query_copy(step):
        return pltpu.make_async_remote_copy(
            src_ref=queries_ref,
            dst_ref=all_queries.at[group_index],
            send_sem=query_send.at[step],
            recv_sem=query_recv.at[step],
            device_id={"grp": xor_index(group_index, step)},
            device_id_type=MESH,
        )

    def scale_copy(step):
        return pltpu.make_async_remote_copy(
            src_ref=block_scale_ref,
            dst_ref=scales_in.at[me],
            send_sem=scale_send.at[step],
            recv_sem=scale_recv.at[step],
            device_id=source_device(xor_index(me, step)),
            device_id_type=MESH,
        )

    own_scales = pltpu.make_async_copy(block_scale_ref, scales_in.at[me], local_sems.at[1])

    def block_copy(plane, step):
        other = xor_index(me, step)
        return pltpu.make_async_remote_copy(
            src_ref=send.at[plane, other],
            dst_ref=arrived[plane].at[pl.ds(me * capacity, capacity)],
            send_sem=block_send.at[plane, step],
            recv_sem=block_recv.at[plane, step],
            device_id=source_device(other),
            device_id_type=MESH,
        )

    def own_blocks(plane):
        return pltpu.make_async_copy(
            send.at[plane, me],
            arrived[plane].at[pl.ds(me * capacity, capacity)],
            local_sems.at[2 + plane],
        )

    steps = sorted(range(1, sources), key=lambda s: (s // group_count == 0, s % group_count, s))
    near_steps = [s for s in steps if (s // group_count).bit_count() <= 1]
    far_steps = [s for s in steps if s not in near_steps]

    tail_plane, tail_step = planes - 1, far_steps[-1] if far_steps else 0
    kept = capacity - tail_blocks.shape[0]
    origin = (seq_count - 1) * group_count
    to_relay = group_count * (1 << max(tail_step // group_count, 1).bit_length() - 1)
    to_relay += tail_step % group_count
    hands_over = me == origin
    relays = me == origin ^ to_relay

    def far_copy(plane, step):
        if (plane, step) != (tail_plane, tail_step):
            return block_copy(plane, step)
        other = xor_index(me, step)
        return pltpu.make_async_remote_copy(
            src_ref=send.at[plane, other, pl.ds(0, kept)],
            dst_ref=arrived[plane].at[pl.ds(me * capacity, kept)],
            send_sem=block_send.at[plane, step],
            recv_sem=block_recv.at[plane, step],
            device_id=source_device(other),
            device_id_type=MESH,
        )

    def tail_copy(source, owner, route, sent, received):
        return pltpu.make_async_remote_copy(
            src_ref=source,
            dst_ref=arrived[tail_plane].at[
                pl.ds(owner * capacity + kept, capacity - kept)
            ],
            send_sem=sent,
            recv_sem=received,
            device_id=source_device(xor_index(me, route)),
            device_id_type=MESH,
        )

    if far_steps:
        tail_source = send.at[tail_plane, xor_index(me, tail_step), pl.ds(kept, capacity - kept)]
        tail_direct = tail_copy(
            tail_source, me, tail_step, tail_sems.at[0], tail_sems.at[1]
        )
        tail_passed = tail_copy(
            tail_blocks,
            xor_index(me, to_relay),
            tail_step ^ to_relay,
            tail_sems.at[2],
            tail_sems.at[1],
        )
        tail_handed = pltpu.make_async_remote_copy(
            src_ref=tail_source,
            dst_ref=tail_blocks,
            send_sem=tail_sems.at[3],
            recv_sem=tail_sems.at[4],
            device_id=source_device(xor_index(me, to_relay)),
            device_id_type=MESH,
        )

    def picked(other, within, request):
        group = other % group_count
        return pick_words[within, group * per_group + request, other // group_count]

    def slot_of(other, within):
        slot = slot_words[within, other % group_count * seq_count + other // group_count]
        return jnp.clip(slot, 0, pool_slots - 1)

    def sort_blocks(plane, other):
        def place(within, _):
            send[plane, other, within] = raw[plane][slot_of(other, within)]
            return 0

        lax.fori_loop(0, capacity, place, 0)

    def sort_plane(plane):
        def place(other, _):
            sort_blocks(plane, other)
            return 0

        lax.fori_loop(0, sources, place, 0)

    def send_plane(plane, chosen):
        for step in chosen:
            block_copy(plane, step).start()

    slot_copy.wait()
    pool_load(0).wait()
    for place, step in enumerate(near_steps):
        other = xor_index(me, step)
        for within in range(capacity):
            send[0, other, within] = raw[0][slot_of(other, within)]
        if place:
            block_copy(0, near_steps[place - 1]).start()
    sort_blocks(0, me)
    block_copy(0, near_steps[-1]).start()
    for copy in small_loads:
        copy.start()
    for plane in range(1, planes):
        pool_load(plane).start()
    for copy in small_loads:
        copy.wait()
    own_queries.start()
    for step in range(1, group_count):
        query_copy(step).start()
    for step in steps:
        scale_copy(step).start()
    own_scales.start()
    weight_load = pltpu.make_async_copy(weight_ref, weights, load_sems.at[planes])
    weight_load.start()
    for step in far_steps:
        sort_blocks(0, xor_index(me, step))
    for plane in range(1, planes):
        pool_load(plane).wait()
        sort_plane(plane)
        if plane == 1:
            send_plane(plane, near_steps)
    if far_steps:
        pl.when(hands_over)(tail_handed.start)
    for plane in range(planes):
        own_blocks(plane).start()

    arrival = jnp.zeros(wide, f32)
    for source in range(sources):
        theirs = owner == source
        arrival = jnp.where(theirs, ranks(theirs) + source * capacity, arrival)
    arrival_rows[...] = arrival.astype(jnp.int32)
    context = jnp.full(wide, lengths_ref[0], jnp.int32)
    for request in range(1, batch_rows):
        context = jnp.where(row_of == request, lengths_ref[request], context)
    live = jnp.clip(context - col_of * block_size, 0, block_size).astype(f32)
    scales_wide[...] = block_scale_ref[...].astype(f32)
    word_copies = [
        pick(live),
        pltpu.make_async_copy(arrival_rows, arrival_words, word_sems.at[2]),
        pltpu.make_async_copy(scales_wide, scale_words, word_sems.at[3]),
    ]
    for copy in word_copies:
        copy.start()
    for copy in word_copies:
        copy.wait()

    own_queries.wait()
    for step in range(1, group_count):
        query_copy(step).wait()

    lanes = lax.broadcasted_iota(jnp.int32, (query_rows, block_size), 1)
    row_ids = lax.broadcasted_iota(jnp.int32, (query_rows, block_size), 0)
    share_lanes = lax.broadcasted_iota(jnp.int32, (row_share, head_size), 1)
    share_rows = lax.broadcasted_iota(jnp.int32, (row_share, head_size), 0)
    for head in range(key_heads):
        peaks[...] = jnp.full_like(peaks, absent_score)
        sums[...] = jnp.zeros_like(sums)
        accums[...] = jnp.zeros_like(accums)

        def score_blocks(other, _):
            group = other % group_count
            keys = send[2 * head, other].reshape(capacity * block_size, head_size)
            raw_scores = lax.dot_general(
                all_queries[group, head],
                keys,
                (((1,), (1,)), ((), ())),
                preferred_element_type=jnp.float32,
            )
            highest = peaks[group]
            for within in range(capacity):
                limit = jnp.full(lanes.shape, picked(other, within, 0), jnp.int32)
                for request in range(1, per_group):
                    limit = jnp.where(
                        row_ids >= request * groups, picked(other, within, request), limit
                    )
                part = raw_scores[:, within * block_size : (within + 1) * block_size]
                part = part * scale_words[2 * head, slot_of(other, within)] * root_scale
                part = jnp.where(lanes < limit, part, absent_score)
                scores[other, :, within * block_size : (within + 1) * block_size] = part
                highest = jnp.maximum(highest, part)
            peaks[group] = highest
            return 0

        lax.fori_loop(0, sources, score_blocks, 0)
        for group in range(group_count):
            peaks[group] = jnp.broadcast_to(
                jnp.max(peaks[group], axis=1, keepdims=True), lanes.shape
            )

        def weigh_blocks(other, _):
            group = other % group_count
            peak = peaks[group]
            total = sums[group]
            pieces = []
            for within in range(capacity):
                part = scores[other, :, within * block_size : (within + 1) * block_size]
                weight = jnp.where(part > absent_limit, jnp.exp(part - peak), 0.0)
                total = total + weight
                pieces.append(
                    (weight * scale_words[2 * head + 1, slot_of(other, within)]).astype(bf16)
                )
            sums[group] = total
            values = send[2 * head + 1, other].reshape(capacity * block_size, head_size)
            accums[group] += jnp.dot(
                jnp.concatenate(pieces, axis=1), values, preferred_element_type=jnp.float32
            )
            return 0

        lax.fori_loop(0, sources, weigh_blocks, 0)
        for group in range(group_count):
            total = jnp.broadcast_to(jnp.sum(sums[group], axis=1, keepdims=True), lanes.shape)
            for request in range(per_group):
                tile = (group * key_heads + head) * per_group + request
                for piece in range(per_tile):
                    low = request * groups + piece * row_share
                    place = tile * per_tile + piece
                    parts[place] = accums[group, low : low + row_share].astype(bf16)
                    stats[place] = jnp.sum(
                        jnp.where(
                            share_lanes == share_rows, peaks[group, low : low + row_share], 0.0
                        )
                        + jnp.where(
                            share_lanes == share_rows + row_share,
                            total[low : low + row_share],
                            0.0,
                        ),
                        axis=0,
                        keepdims=True,
                    )

    def part_copy(step):
        other = xor_index(me, step)
        return pltpu.make_async_remote_copy(
            src_ref=parts.at[other],
            dst_ref=parts_in.at[me],
            send_sem=part_send.at[step],
            recv_sem=part_recv.at[step],
            device_id=source_device(other),
            device_id_type=MESH,
        )

    def stat_copy(step):
        other = xor_index(me, step)
        return pltpu.make_async_remote_copy(
            src_ref=stats.at[other],
            dst_ref=stats_in.at[me],
            send_sem=stat_send.at[step],
            recv_sem=stat_recv.at[step],
            device_id=source_device(other),
            device_id_type=MESH,
        )

    for step in steps:
        stat_copy(step).start()
        part_copy(step).start()
    parts_in[me] = parts[me]
    stats_in[me] = stats[me]
    for plane in range(2, min(planes, 3)):
        send_plane(plane, near_steps)

    @pl.when(below)
    def _():
        pl.semaphore_signal(
            known_above.at[0], inc=1, device_id={"tp": tp_index - 1}, device_id_type=MESH
        )

    @pl.when(above)
    def _():
        pl.semaphore_wait(known_above.at[0], 1)

    for reach in range(1, tp_count - 1):

        @pl.when(jnp.logical_and(tp_index >= reach, above))
        def _():
            pl.semaphore_signal(
                known_below.at[reach], inc=1, device_id={"tp": tp_index + 1}, device_id_type=MESH
            )

        @pl.when(jnp.logical_and(tp_index + reach < tp_count, below))
        def _():
            pl.semaphore_signal(
                known_above.at[reach], inc=1, device_id={"tp": tp_index - 1}, device_id_type=MESH
            )

        @pl.when(tp_index - 1 >= reach)
        def _():
            pl.semaphore_wait(known_below.at[reach], 1)

        @pl.when(tp_index + 1 + reach < tp_count)
        def _():
            pl.semaphore_wait(known_above.at[reach], 1)

    for step in steps:
        stat_copy(step).wait_recv()
        part_copy(step).wait_recv()

    def spread(source, first):
        return jnp.broadcast_to(
            jnp.sum(
                jnp.where(
                    share_lanes == share_rows + first,
                    jnp.broadcast_to(stats_in[source], share_lanes.shape),
                    0.0,
                ),
                axis=1,
                keepdims=True,
            ),
            share_lanes.shape,
        )

    source_peaks = [spread(source, 0) for source in range(sources)]
    highest = functools.reduce(jnp.maximum, source_peaks)
    numerator = jnp.zeros_like(highest)
    denominator = jnp.zeros_like(highest)
    for source in range(sources):
        factor = jnp.exp(source_peaks[source] - highest)
        numerator += parts_in[source].astype(f32) * factor
        denominator += spread(source, row_share) * factor
    attended[me] = (numerator / denominator).astype(jnp.bfloat16)

    def att_copy(step):
        return pltpu.make_async_remote_copy(
            src_ref=attended.at[me],
            dst_ref=attended.at[me],
            send_sem=att_send.at[step],
            recv_sem=att_recv.at[step],
            device_id=source_device(xor_index(me, step)),
            device_id_type=MESH,
        )

    weight_load.wait()
    for step in steps:
        att_copy(step).start()
    for plane in range(3, planes):
        send_plane(plane, near_steps)
    for step in steps:
        att_copy(step).wait_recv()
    for plane in range(planes):
        for step in near_steps:
            if step // group_count == 1:
                block_copy(plane, step).wait_send()
    if far_steps:

        @pl.when(relays)
        def _():
            tail_handed.wait_recv()
            tail_passed.start()

    for plane in range(planes):
        for step in far_steps:
            far_copy(plane, step).start()
    if far_steps:
        pl.when(jnp.logical_not(hands_over))(tail_direct.start)

    rows = sources * row_share
    gathered = attended[...].astype(f32).reshape(rows, head_size)
    row = lax.broadcasted_iota(jnp.int32, (rows, head_size), 0)
    row_head = (row // (groups * per_group)) % key_heads * groups + row % groups
    left = jnp.concatenate(
        [
            jnp.where(row_head == head, gathered, 0.0).astype(jnp.bfloat16)
            for head in range(key_heads * groups)
        ],
        axis=1,
    )
    columns = weights.shape[1]
    width = min(columns, 256)
    here = batch_rows // tp_count
    for low in range(0, columns, width):
        product = jnp.dot(left, weights[:, low : low + width], preferred_element_type=jnp.float32)
        for request in range(batch_rows):
            group, inner = request // per_group, request % per_group
            total = jnp.zeros((1, width), jnp.float32)
            for head in range(key_heads):
                tile = (group * key_heads + head) * per_group + inner
                total += jnp.sum(
                    product[tile * groups : (tile + 1) * groups], axis=0, keepdims=True
                )
            projected[request // here, pl.ds(request % here, 1), low : low + width] = total

    def proj_copy(step):
        other = xor_index(tp_index, step)
        return pltpu.make_async_remote_copy(
            src_ref=projected.at[other],
            dst_ref=projected_in.at[tp_index],
            send_sem=proj_send.at[step],
            recv_sem=proj_recv.at[step],
            device_id={"tp": other},
            device_id_type=MESH,
        )

    for step in range(1, tp_count):
        proj_copy(step).start()
    projected_in[tp_index] = projected[tp_index]
    for step in range(1, tp_count):
        proj_copy(step).wait()
    total = projected_in[0]
    for source in range(1, tp_count):
        total += projected_in[source]
    output_ref[...] = total.astype(output_ref.dtype)

    own_scales.wait()
    for step in steps:
        scale_copy(step).wait()
    slot_ids = lax.broadcasted_iota(jnp.int32, (pool_slots, table_width), 0)
    wanted = jnp.where(
        lax.broadcasted_iota(jnp.int32, (table_width, share_blocks), 0)
        == lax.broadcasted_iota(jnp.int32, (table_width, share_blocks), 1)
        + seq_index * share_blocks,
        1.0,
        0.0,
    ).astype(bf16)
    for request in range(per_group):
        slots = table_ref[pl.ds(group_index * per_group + request, 1), :]
        found = jnp.zeros((planes, table_width), f32)
        for source in range(sources):
            onehot = jnp.where(slots == slot_ids + source * pool_slots, 1.0, 0.0).astype(bf16)
            found += jnp.dot(scales_in[source], onehot, preferred_element_type=f32)
        scales_out_ref[request] = jnp.dot(
            found.astype(bf16), wanted, preferred_element_type=f32
        ).astype(bf16)

    unroll = 4 if share_blocks % 4 == 0 else 1
    for plane in range(planes - 1):
        own_blocks(plane).wait()
        for step in steps:
            (block_copy if step in near_steps else far_copy)(plane, step).wait_recv()
        for request in range(per_group):

            def place(turn, _):
                for part in range(unroll):
                    column = turn * unroll + part
                    index = arrival_words[
                        group_index * per_group + request, seq_index * share_blocks + column
                    ]
                    placed_ref[request * share_blocks + column, plane] = arrived[plane][
                        jnp.clip(index, 0, positions - 1)
                    ]
                return 0

            lax.fori_loop(0, share_blocks // unroll, place, 0)
    for step in steps:
        part_copy(step).wait_send()
        stat_copy(step).wait_send()
        att_copy(step).wait_send()
    own_blocks(planes - 1).wait()
    for step in near_steps:
        block_copy(planes - 1, step).wait_recv()
    for plane in range(planes):
        for step in far_steps:
            far_copy(plane, step).wait_send()
    for plane in range(planes):
        for step in near_steps:
            if step // group_count != 1:
                block_copy(plane, step).wait_send()
    if far_steps:
        pl.when(hands_over)(tail_handed.wait_send)
        pl.when(relays)(tail_passed.wait_send)
        pl.when(jnp.logical_not(hands_over))(tail_direct.wait_send)
    for step in far_steps:
        far_copy(planes - 1, step).wait_recv()
    if far_steps:
        tail_direct.wait_recv()


def copy_out_kernel(
    placed_in,
    last_in,
    arrival_in,
    scale_in,
    output_in,
    cache_ref,
    scale_ref,
    output_ref,
    arrival_words,
    sems,
    block_sem,
):
    positions, first = placed_in.shape[:2]
    per_group, _, share_blocks = scale_in.shape
    group_index, seq_index = lax.axis_index("grp"), lax.axis_index("seq")
    words = pltpu.make_async_copy(arrival_in, arrival_words, sems.at[0])
    words.start()
    chunks = 8
    share = positions // chunks
    copies = [
        pltpu.make_async_copy(
            placed_in.at[pl.ds(part * share, share)],
            cache_ref.at[pl.ds(part * share, share), pl.ds(0, first)],
            sems.at[3 + part],
        )
        for part in range(chunks)
    ]
    copies.append(pltpu.make_async_copy(scale_in, scale_ref, sems.at[1]))
    copies.append(pltpu.make_async_copy(output_in, output_ref, sems.at[2]))
    for copy in copies:
        copy.start()
    words.wait()

    def block(position):
        index = arrival_words[
            group_index * per_group + position // share_blocks,
            seq_index * share_blocks + position % share_blocks,
        ]
        return pltpu.make_async_copy(
            last_in.at[jnp.clip(index, 0, positions - 1)],
            cache_ref.at[position, first],
            block_sem,
        )

    def start(position, _):
        block(position).start()
        return 0

    lax.fori_loop(0, positions, start, 0, unroll=4)
    for copy in copies:
        copy.wait()
    pltpu.make_async_copy(last_in, cache_ref.at[:, first], block_sem).wait()


def per_device(queries, cache_pool, block_scale, block_table, lengths, output_weight):
    seq_count = lax.axis_size("seq")
    group_count = lax.axis_size("grp")
    tp_count = lax.axis_size("tp")
    sources = seq_count * group_count
    pool_slots, key_heads, _, block_size, head_size = cache_pool.shape
    batch_rows, table_width = block_table.shape
    per_group = batch_rows // group_count
    share_blocks = table_width // seq_count
    capacity = pool_slots // sources
    heads_here = queries.shape[1]
    groups = heads_here // key_heads
    planes = key_heads * 2
    positions = per_group * share_blocks
    columns = output_weight.shape[1]
    root_scale = 1.0 / math.sqrt(head_size)

    row_share = batch_rows * key_heads * groups // sources
    query_rows = per_group * groups
    f32, bf16 = jnp.float32, jnp.bfloat16
    dma = pltpu.SemaphoreType.DMA
    vmem = pl.BlockSpec(memory_space=pltpu.VMEM)
    hbm = pl.BlockSpec(memory_space=pltpu.HBM)
    here = batch_rows // tp_count
    results = pl.pallas_call(
        functools.partial(
            exchange_kernel, (seq_count, group_count, tp_count, per_group, root_scale)
        ),
        out_shape=(
            pltpu.VMEM((positions, planes - 1, block_size, head_size), bf16),
            pltpu.VMEM((positions, block_size, head_size), bf16),
            pltpu.VMEM((batch_rows, table_width), jnp.int32),
            pltpu.VMEM((per_group, planes, share_blocks), bf16),
            pltpu.VMEM((here, columns), bf16),
        ),
        in_specs=[hbm, hbm, hbm, hbm, hbm, hbm],
        out_specs=(vmem,) * 5,
        scratch_shapes=[
            pltpu.SMEM((batch_rows,), jnp.int32),
            pltpu.VMEM((batch_rows, table_width), jnp.int32),
            pltpu.VMEM((planes, pool_slots), bf16),
            pltpu.VMEM((key_heads, query_rows, head_size), bf16),
            [pltpu.VMEM((pool_slots, block_size, head_size), bf16) for _ in range(planes)],
            pltpu.VMEM((planes, sources, capacity, block_size, head_size), bf16),
            [pltpu.VMEM((pool_slots, block_size, head_size), bf16) for _ in range(planes - 1)],
            pltpu.VMEM((heads_here * head_size, columns), bf16),
            pltpu.VMEM((group_count, key_heads, query_rows, head_size), bf16),
            pltpu.VMEM((sources, query_rows, capacity * block_size), f32),
            pltpu.VMEM((group_count, query_rows, block_size), f32),
            pltpu.VMEM((group_count, query_rows, block_size), f32),
            pltpu.VMEM((group_count, query_rows, head_size), f32),
            pltpu.VMEM((sources, row_share, head_size), bf16),
            pltpu.VMEM((sources, row_share, head_size), bf16),
            pltpu.VMEM((sources, 1, head_size), f32),
            pltpu.VMEM((sources, 1, head_size), f32),
            pltpu.VMEM((sources, row_share, head_size), bf16),
            pltpu.VMEM((tp_count, here, columns), f32),
            pltpu.VMEM((tp_count, here, columns), f32),
            pltpu.VMEM((sources, planes, pool_slots), bf16),
            pltpu.VMEM((planes, pool_slots), f32),
            pltpu.VMEM((capacity, batch_rows, table_width), jnp.int32),
            pltpu.SMEM((planes, pool_slots), f32),
            pltpu.SMEM((batch_rows, table_width), jnp.int32),
            pltpu.SMEM((capacity, batch_rows, table_width), jnp.int32),
            pltpu.VMEM((capacity, table_width), jnp.int32),
            pltpu.SMEM((capacity, table_width), jnp.int32),
            dma((planes + 1,)),
            dma((planes + 3,)),
            dma((7 + key_heads * per_group,)),
            dma((planes, sources)),
            dma((planes, sources)),
            pltpu.VMEM((max(capacity // 4, 1), block_size, head_size), bf16),
            dma((5,)),
            dma((group_count,)),
            dma((group_count,)),
            dma((sources,)),
            dma((sources,)),
            dma((sources,)),
            dma((sources,)),
            dma((sources,)),
            dma((sources,)),
            pltpu.SemaphoreType.REGULAR((tp_count,)),
            pltpu.SemaphoreType.REGULAR((tp_count,)),
            dma((sources,)),
            dma((sources,)),
            dma((tp_count,)),
            dma((tp_count,)),
        ],
        compiler_params=pltpu.CompilerParams(
            collective_id=0, has_side_effects=True, vmem_limit_bytes=40 * 2**20
        ),
    )(
        *(
            pltpu.with_memory_space_constraint(operand, pltpu.HBM)
            for operand in (
                lengths,
                block_table,
                block_scale.reshape(pool_slots, planes).T,
                queries,
                cache_pool.reshape(pool_slots, planes, block_size, head_size),
                output_weight,
            )
        )
    )
    decode_cache, decode_scale, output = pl.pallas_call(
        copy_out_kernel,
        out_shape=(
            jax.ShapeDtypeStruct((positions, planes, block_size, head_size), bf16),
            jax.ShapeDtypeStruct(results[3].shape, bf16),
            jax.ShapeDtypeStruct(results[4].shape, bf16),
        ),
        in_specs=[vmem] * 5,
        out_specs=(hbm,) * 3,
        scratch_shapes=[
            pltpu.SMEM((batch_rows, table_width), jnp.int32),
            dma((11,)),
            dma,
        ],
        compiler_params=pltpu.CompilerParams(vmem_limit_bytes=16 * 2**20),
    )(*(pltpu.with_memory_space_constraint(r, pltpu.VMEM) for r in results))
    return (
        output,
        decode_cache.reshape(per_group, share_blocks, key_heads, 2, block_size, head_size),
        decode_scale.transpose(0, 2, 1).reshape(per_group, share_blocks, key_heads, 2),
    )


def solution(mesh):
    placed = (
        P("grp", "tp", None),
        P(("seq", "grp"), "tp", None, None, None),
        P(("seq", "grp"), "tp", None),
        P(),
        P(),
        P("tp", ("seq", "grp")),
    )
    return jax.shard_map(
        per_device,
        mesh=mesh,
        in_specs=placed,
        out_specs=(
            P("tp", ("seq", "grp")),
            P("grp", "seq", "tp", None, None, None),
            P("grp", "seq", "tp", None),
        ),
        check_vma=False,
    )
```

```python
import functools
import math

import jax
import jax.numpy as jnp
from jax import lax
from jax.experimental import pallas as pl
from jax.experimental.pallas import tpu as pltpu
from jax.sharding import PartitionSpec as P

MESH = pl.DeviceIdType.MESH
absent_score = -1e30
absent_limit = -1e29


def xor_index(index, mask):
    out = index
    bit = 1
    while bit <= mask:
        if mask & bit:
            out = out + bit - 2 * bit * ((index // bit) % 2)
        bit *= 2
    return out


def exchange_kernel(
    dims,
    lengths_in,
    table_in,
    block_scale_in,
    queries_in,
    pool_ref,
    weight_ref,
    placed_ref,
    last_ref,
    arrival_rows,
    scales_out_ref,
    output_ref,
    lengths_ref,
    table_ref,
    block_scale_ref,
    queries_ref,
    raw,
    send,
    arrived,
    weights,
    all_queries,
    scores,
    peaks,
    sums,
    accums,
    parts,
    parts_in,
    stats,
    stats_in,
    attended,
    projected,
    projected_in,
    scales_in,
    scales_wide,
    pick_rows,
    scale_words,
    arrival_words,
    pick_words,
    slot_rows,
    slot_words,
    load_sems,
    local_sems,
    word_sems,
    block_send,
    block_recv,
    tail_blocks,
    tail_sems,
    query_send,
    query_recv,
    scale_send,
    scale_recv,
    part_send,
    part_recv,
    stat_send,
    stat_recv,
    known_below,
    known_above,
    att_send,
    att_recv,
    proj_send,
    proj_recv,
):
    seq_count, group_count, tp_count, per_group, root_scale = dims
    sources = seq_count * group_count
    seq_index = lax.axis_index("seq")
    group_index = lax.axis_index("grp")
    tp_index = lax.axis_index("tp")
    me = seq_index * group_count + group_index
    planes, _, capacity, block_size, head_size = send.shape
    arrived = [*arrived, last_ref]
    pool_slots = raw[0].shape[0]
    key_heads = planes // 2
    query_rows = all_queries.shape[2]
    groups = query_rows // per_group
    batch_rows, table_width = table_ref.shape
    share_blocks = table_width // seq_count
    positions = per_group * share_blocks
    row_share = parts.shape[1]
    per_tile = groups // row_share
    f32, bf16 = jnp.float32, jnp.bfloat16

    def pool_load(plane):
        return pltpu.make_async_copy(pool_ref.at[:, plane], raw[plane], load_sems.at[plane])

    table_load = pltpu.make_async_copy(table_in, table_ref, word_sems.at[4])
    small_loads = [
        pltpu.make_async_copy(lengths_in, lengths_ref, word_sems.at[5]),
        pltpu.make_async_copy(block_scale_in, block_scale_ref, word_sems.at[6]),
    ] + [
        pltpu.make_async_copy(
            queries_in.at[request, pl.ds(head * groups, groups)],
            queries_ref.at[head, pl.ds(request * groups, groups)],
            word_sems.at[7 + head * per_group + request],
        )
        for head in range(key_heads)
        for request in range(per_group)
    ]
    table_load.start()
    pool_load(0).start()

    def source_device(other):
        return {"seq": other // group_count, "grp": other % group_count}

    barrier = pltpu.get_barrier_semaphore()
    for step in range(1, sources):
        pl.semaphore_signal(
            barrier, inc=1, device_id=source_device(xor_index(me, step)), device_id_type=MESH
        )
    below, above = tp_index > 0, tp_index < tp_count - 1

    @pl.when(above)
    def _():
        pl.semaphore_signal(
            barrier, inc=1, device_id={"tp": tp_index + 1}, device_id_type=MESH
        )

    wide = (batch_rows, table_width)
    table_load.wait()
    table = table_ref[...]
    row_of = lax.broadcasted_iota(jnp.int32, wide, 0)
    col_of = lax.broadcasted_iota(jnp.int32, wide, 1)
    square = (table_width, table_width)
    upper = lax.broadcasted_iota(jnp.int32, square, 0)
    lower = lax.broadcasted_iota(jnp.int32, square, 1)
    alike = upper // share_blocks == lower // share_blocks
    all_alike = jnp.where(alike, 1.0, 0.0).astype(bf16)
    earlier = jnp.where(alike, jnp.where(upper < lower, 1.0, 0.0), 0.0).astype(bf16)
    owner = table // pool_slots
    local = (table % pool_slots).astype(f32)

    def ranks(theirs):
        ones = jnp.where(theirs, 1.0, 0.0).astype(bf16)
        rank = jnp.dot(ones, earlier, preferred_element_type=f32)
        whole = jnp.dot(ones, all_alike, preferred_element_type=f32)
        for request in range(batch_rows):
            last = request // per_group * per_group + per_group
            for later in range(request + 1, last):
                rank = rank + jnp.where(row_of == later, whole[request : request + 1], 0.0)
        return rank

    range_of = jnp.where(upper // share_blocks == lower, 1.0, 0.0).astype(bf16)
    own_rank = jnp.where(owner == me, ranks(owner == me), -1.0)

    rank_rows = lax.broadcasted_iota(jnp.int32, (capacity, table_width), 0).astype(f32)
    slots = jnp.zeros((capacity, table_width), f32)
    for request in range(batch_rows):
        column = upper // share_blocks + request // per_group * seq_count
        slots += jnp.dot(
            jnp.where(
                own_rank[request : request + 1] == rank_rows, local[request : request + 1], 0.0
            ).astype(bf16),
            jnp.where(column == lower, 1.0, 0.0).astype(bf16),
            preferred_element_type=f32,
        )
    slot_rows[...] = slots.astype(jnp.int32)
    slot_copy = pltpu.make_async_copy(slot_rows, slot_words, word_sems.at[0])
    slot_copy.start()

    def pick(values):
        for within in range(capacity):
            pick_rows[within] = jnp.dot(
                jnp.where(own_rank == within, values, 0.0).astype(bf16),
                range_of,
                preferred_element_type=f32,
            ).astype(jnp.int32)
        return pltpu.make_async_copy(pick_rows, pick_words, word_sems.at[1])

    own_queries = pltpu.make_async_copy(queries_ref, all_queries.at[group_index], local_sems.at[0])
    pl.semaphore_wait(barrier, sources - 1 + jnp.where(below, 1, 0))

    def query_copy(step):
        return pltpu.make_async_remote_copy(
            src_ref=queries_ref,
            dst_ref=all_queries.at[group_index],
            send_sem=query_send.at[step],
            recv_sem=query_recv.at[step],
            device_id={"grp": xor_index(group_index, step)},
            device_id_type=MESH,
        )

    def scale_copy(step):
        return pltpu.make_async_remote_copy(
            src_ref=block_scale_ref,
            dst_ref=scales_in.at[me],
            send_sem=scale_send.at[step],
            recv_sem=scale_recv.at[step],
            device_id=source_device(xor_index(me, step)),
            device_id_type=MESH,
        )

    own_scales = pltpu.make_async_copy(block_scale_ref, scales_in.at[me], local_sems.at[1])

    def block_copy(plane, step):
        other = xor_index(me, step)
        return pltpu.make_async_remote_copy(
            src_ref=send.at[plane, other],
            dst_ref=arrived[plane].at[pl.ds(me * capacity, capacity)],
            send_sem=block_send.at[plane, step],
            recv_sem=block_recv.at[plane, step],
            device_id=source_device(other),
            device_id_type=MESH,
        )

    def own_blocks(plane):
        return pltpu.make_async_copy(
            send.at[plane, me],
            arrived[plane].at[pl.ds(me * capacity, capacity)],
            local_sems.at[2 + plane],
        )

    steps = sorted(range(1, sources), key=lambda s: (s // group_count == 0, s % group_count, s))
    near_steps = [s for s in steps if (s // group_count).bit_count() <= 1]
    far_steps = [s for s in steps if s not in near_steps]

    tail_plane, tail_step = planes - 1, far_steps[-1] if far_steps else 0
    kept = capacity - tail_blocks.shape[0]
    origin = (seq_count - 1) * group_count
    to_relay = group_count * (1 << max(tail_step // group_count, 1).bit_length() - 1)
    to_relay += tail_step % group_count
    hands_over = me == origin
    relays = me == origin ^ to_relay

    def far_copy(plane, step):
        if (plane, step) != (tail_plane, tail_step):
            return block_copy(plane, step)
        other = xor_index(me, step)
        return pltpu.make_async_remote_copy(
            src_ref=send.at[plane, other, pl.ds(0, kept)],
            dst_ref=arrived[plane].at[pl.ds(me * capacity, kept)],
            send_sem=block_send.at[plane, step],
            recv_sem=block_recv.at[plane, step],
            device_id=source_device(other),
            device_id_type=MESH,
        )

    def tail_copy(source, owner, route, sent, received):
        return pltpu.make_async_remote_copy(
            src_ref=source,
            dst_ref=arrived[tail_plane].at[
                pl.ds(owner * capacity + kept, capacity - kept)
            ],
            send_sem=sent,
            recv_sem=received,
            device_id=source_device(xor_index(me, route)),
            device_id_type=MESH,
        )

    if far_steps:
        tail_source = send.at[tail_plane, xor_index(me, tail_step), pl.ds(kept, capacity - kept)]
        tail_direct = tail_copy(
            tail_source, me, tail_step, tail_sems.at[0], tail_sems.at[1]
        )
        tail_passed = tail_copy(
            tail_blocks,
            xor_index(me, to_relay),
            tail_step ^ to_relay,
            tail_sems.at[2],
            tail_sems.at[1],
        )
        tail_handed = pltpu.make_async_remote_copy(
            src_ref=tail_source,
            dst_ref=tail_blocks,
            send_sem=tail_sems.at[3],
            recv_sem=tail_sems.at[4],
            device_id=source_device(xor_index(me, to_relay)),
            device_id_type=MESH,
        )

    def picked(other, within, request):
        group = other % group_count
        return pick_words[within, group * per_group + request, other // group_count]

    def slot_of(other, within):
        slot = slot_words[within, other % group_count * seq_count + other // group_count]
        return jnp.clip(slot, 0, pool_slots - 1)

    def sort_blocks(plane, other):
        def place(within, _):
            send[plane, other, within] = raw[plane][slot_of(other, within)]
            return 0

        lax.fori_loop(0, capacity, place, 0)

    def sort_plane(plane):
        def place(other, _):
            sort_blocks(plane, other)
            return 0

        lax.fori_loop(0, sources, place, 0)

    def send_plane(plane, chosen):
        for step in chosen:
            block_copy(plane, step).start()

    slot_copy.wait()
    pool_load(0).wait()
    for place, step in enumerate(near_steps):
        other = xor_index(me, step)
        for within in range(capacity):
            send[0, other, within] = raw[0][slot_of(other, within)]
        if place:
            block_copy(0, near_steps[place - 1]).start()
    sort_blocks(0, me)
    block_copy(0, near_steps[-1]).start()
    for copy in small_loads:
        copy.start()
    for plane in range(1, planes):
        pool_load(plane).start()
    for copy in small_loads:
        copy.wait()
    own_queries.start()
    for step in range(1, group_count):
        query_copy(step).start()
    for step in steps:
        scale_copy(step).start()
    own_scales.start()
    weight_load = pltpu.make_async_copy(weight_ref, weights, load_sems.at[planes])
    weight_load.start()
    for step in far_steps:
        sort_blocks(0, xor_index(me, step))
    for plane in range(1, planes):
        pool_load(plane).wait()
        sort_plane(plane)
        if plane == 1:
            send_plane(plane, near_steps)
    if far_steps:
        pl.when(hands_over)(tail_handed.start)
    for plane in range(planes):
        own_blocks(plane).start()

    arrival = jnp.zeros(wide, f32)
    for source in range(sources):
        theirs = owner == source
        arrival = jnp.where(theirs, ranks(theirs) + source * capacity, arrival)
    arrival_rows[...] = arrival.astype(jnp.int32)
    context = jnp.full(wide, lengths_ref[0], jnp.int32)
    for request in range(1, batch_rows):
        context = jnp.where(row_of == request, lengths_ref[request], context)
    live = jnp.clip(context - col_of * block_size, 0, block_size).astype(f32)
    scales_wide[...] = block_scale_ref[...].astype(f32)
    word_copies = [
        pick(live),
        pltpu.make_async_copy(arrival_rows, arrival_words, word_sems.at[2]),
        pltpu.make_async_copy(scales_wide, scale_words, word_sems.at[3]),
    ]
    for copy in word_copies:
        copy.start()
    for copy in word_copies:
        copy.wait()

    own_queries.wait()
    for step in range(1, group_count):
        query_copy(step).wait()

    lanes = lax.broadcasted_iota(jnp.int32, (query_rows, block_size), 1)
    row_ids = lax.broadcasted_iota(jnp.int32, (query_rows, block_size), 0)
    share_lanes = lax.broadcasted_iota(jnp.int32, (row_share, head_size), 1)
    share_rows = lax.broadcasted_iota(jnp.int32, (row_share, head_size), 0)
    for head in range(key_heads):
        peaks[...] = jnp.full_like(peaks, absent_score)
        sums[...] = jnp.zeros_like(sums)
        accums[...] = jnp.zeros_like(accums)

        def score_blocks(other, _):
            group = other % group_count
            keys = send[2 * head, other].reshape(capacity * block_size, head_size)
            raw_scores = lax.dot_general(
                all_queries[group, head],
                keys,
                (((1,), (1,)), ((), ())),
                preferred_element_type=jnp.float32,
            )
            highest = peaks[group]
            for within in range(capacity):
                limit = jnp.full(lanes.shape, picked(other, within, 0), jnp.int32)
                for request in range(1, per_group):
                    limit = jnp.where(
                        row_ids >= request * groups, picked(other, within, request), limit
                    )
                part = raw_scores[:, within * block_size : (within + 1) * block_size]
                part = part * scale_words[2 * head, slot_of(other, within)] * root_scale
                part = jnp.where(lanes < limit, part, absent_score)
                scores[other, :, within * block_size : (within + 1) * block_size] = part
                highest = jnp.maximum(highest, part)
            peaks[group] = highest
            return 0

        lax.fori_loop(0, sources, score_blocks, 0)
        for group in range(group_count):
            peaks[group] = jnp.broadcast_to(
                jnp.max(peaks[group], axis=1, keepdims=True), lanes.shape
            )

        def weigh_blocks(other, _):
            group = other % group_count
            peak = peaks[group]
            total = sums[group]
            pieces = []
            for within in range(capacity):
                part = scores[other, :, within * block_size : (within + 1) * block_size]
                weight = jnp.where(part > absent_limit, jnp.exp(part - peak), 0.0)
                total = total + weight
                pieces.append(
                    (weight * scale_words[2 * head + 1, slot_of(other, within)]).astype(bf16)
                )
            sums[group] = total
            values = send[2 * head + 1, other].reshape(capacity * block_size, head_size)
            accums[group] += jnp.dot(
                jnp.concatenate(pieces, axis=1), values, preferred_element_type=jnp.float32
            )
            return 0

        lax.fori_loop(0, sources, weigh_blocks, 0)
        for group in range(group_count):
            total = jnp.broadcast_to(jnp.sum(sums[group], axis=1, keepdims=True), lanes.shape)
            for request in range(per_group):
                tile = (group * key_heads + head) * per_group + request
                for piece in range(per_tile):
                    low = request * groups + piece * row_share
                    place = tile * per_tile + piece
                    parts[place] = accums[group, low : low + row_share]
                    stats[place] = jnp.sum(
                        jnp.where(
                            share_lanes == share_rows, peaks[group, low : low + row_share], 0.0
                        )
                        + jnp.where(
                            share_lanes == share_rows + row_share,
                            total[low : low + row_share],
                            0.0,
                        ),
                        axis=0,
                        keepdims=True,
                    )

    def part_copy(step):
        other = xor_index(me, step)
        return pltpu.make_async_remote_copy(
            src_ref=parts.at[other],
            dst_ref=parts_in.at[me],
            send_sem=part_send.at[step],
            recv_sem=part_recv.at[step],
            device_id=source_device(other),
            device_id_type=MESH,
        )

    def stat_copy(step):
        other = xor_index(me, step)
        return pltpu.make_async_remote_copy(
            src_ref=stats.at[other],
            dst_ref=stats_in.at[me],
            send_sem=stat_send.at[step],
            recv_sem=stat_recv.at[step],
            device_id=source_device(other),
            device_id_type=MESH,
        )

    for step in steps:
        stat_copy(step).start()
        part_copy(step).start()
    parts_in[me] = parts[me]
    stats_in[me] = stats[me]
    for plane in range(2, min(planes, 3)):
        send_plane(plane, near_steps)

    @pl.when(below)
    def _():
        pl.semaphore_signal(
            known_above.at[0], inc=1, device_id={"tp": tp_index - 1}, device_id_type=MESH
        )

    @pl.when(above)
    def _():
        pl.semaphore_wait(known_above.at[0], 1)

    for reach in range(1, tp_count - 1):

        @pl.when(jnp.logical_and(tp_index >= reach, above))
        def _():
            pl.semaphore_signal(
                known_below.at[reach], inc=1, device_id={"tp": tp_index + 1}, device_id_type=MESH
            )

        @pl.when(jnp.logical_and(tp_index + reach < tp_count, below))
        def _():
            pl.semaphore_signal(
                known_above.at[reach], inc=1, device_id={"tp": tp_index - 1}, device_id_type=MESH
            )

        @pl.when(tp_index - 1 >= reach)
        def _():
            pl.semaphore_wait(known_below.at[reach], 1)

        @pl.when(tp_index + 1 + reach < tp_count)
        def _():
            pl.semaphore_wait(known_above.at[reach], 1)

    for step in steps:
        stat_copy(step).wait_recv()
        part_copy(step).wait_recv()

    def spread(source, first):
        return jnp.broadcast_to(
            jnp.sum(
                jnp.where(
                    share_lanes == share_rows + first,
                    jnp.broadcast_to(stats_in[source], share_lanes.shape),
                    0.0,
                ),
                axis=1,
                keepdims=True,
            ),
            share_lanes.shape,
        )

    source_peaks = [spread(source, 0) for source in range(sources)]
    highest = functools.reduce(jnp.maximum, source_peaks)
    numerator = jnp.zeros_like(highest)
    denominator = jnp.zeros_like(highest)
    for source in range(sources):
        factor = jnp.exp(source_peaks[source] - highest)
        numerator += parts_in[source] * factor
        denominator += spread(source, row_share) * factor
    attended[me] = (numerator / denominator).astype(jnp.bfloat16)

    def att_copy(step):
        return pltpu.make_async_remote_copy(
            src_ref=attended.at[me],
            dst_ref=attended.at[me],
            send_sem=att_send.at[step],
            recv_sem=att_recv.at[step],
            device_id=source_device(xor_index(me, step)),
            device_id_type=MESH,
        )

    weight_load.wait()
    for step in steps:
        att_copy(step).start()
    for plane in range(3, planes):
        send_plane(plane, near_steps)
    for step in steps:
        att_copy(step).wait_recv()
    for plane in range(planes):
        for step in near_steps:
            if step // group_count == 1:
                block_copy(plane, step).wait_send()
    if far_steps:

        @pl.when(relays)
        def _():
            tail_handed.wait_recv()
            tail_passed.start()

    for plane in range(planes):
        for step in far_steps:
            far_copy(plane, step).start()
    if far_steps:
        pl.when(jnp.logical_not(hands_over))(tail_direct.start)

    rows = sources * row_share
    gathered = attended[...].astype(f32).reshape(rows, head_size)
    row = lax.broadcasted_iota(jnp.int32, (rows, head_size), 0)
    row_head = (row // (groups * per_group)) % key_heads * groups + row % groups
    left = jnp.concatenate(
        [
            jnp.where(row_head == head, gathered, 0.0).astype(jnp.bfloat16)
            for head in range(key_heads * groups)
        ],
        axis=1,
    )
    columns = weights.shape[1]
    width = min(columns, 256)
    here = batch_rows // tp_count
    for low in range(0, columns, width):
        product = jnp.dot(left, weights[:, low : low + width], preferred_element_type=jnp.float32)
        for request in range(batch_rows):
            group, inner = request // per_group, request % per_group
            total = jnp.zeros((1, width), jnp.float32)
            for head in range(key_heads):
                tile = (group * key_heads + head) * per_group + inner
                total += jnp.sum(
                    product[tile * groups : (tile + 1) * groups], axis=0, keepdims=True
                )
            projected[request // here, pl.ds(request % here, 1), low : low + width] = total

    def proj_copy(step):
        other = xor_index(tp_index, step)
        return pltpu.make_async_remote_copy(
            src_ref=projected.at[other],
            dst_ref=projected_in.at[tp_index],
            send_sem=proj_send.at[step],
            recv_sem=proj_recv.at[step],
            device_id={"tp": other},
            device_id_type=MESH,
        )

    for step in range(1, tp_count):
        proj_copy(step).start()
    projected_in[tp_index] = projected[tp_index]
    for step in range(1, tp_count):
        proj_copy(step).wait()
    total = projected_in[0]
    for source in range(1, tp_count):
        total += projected_in[source]
    output_ref[...] = total.astype(output_ref.dtype)

    own_scales.wait()
    for step in steps:
        scale_copy(step).wait()
    slot_ids = lax.broadcasted_iota(jnp.int32, (pool_slots, table_width), 0)
    wanted = jnp.where(
        lax.broadcasted_iota(jnp.int32, (table_width, share_blocks), 0)
        == lax.broadcasted_iota(jnp.int32, (table_width, share_blocks), 1)
        + seq_index * share_blocks,
        1.0,
        0.0,
    ).astype(bf16)
    for request in range(per_group):
        slots = table_ref[pl.ds(group_index * per_group + request, 1), :]
        found = jnp.zeros((planes, table_width), f32)
        for source in range(sources):
            onehot = jnp.where(slots == slot_ids + source * pool_slots, 1.0, 0.0).astype(bf16)
            found += jnp.dot(scales_in[source], onehot, preferred_element_type=f32)
        scales_out_ref[request] = jnp.dot(
            found.astype(bf16), wanted, preferred_element_type=f32
        ).astype(bf16)

    unroll = 4 if share_blocks % 4 == 0 else 1
    for plane in range(planes - 1):
        own_blocks(plane).wait()
        for step in steps:
            (block_copy if step in near_steps else far_copy)(plane, step).wait_recv()
        for request in range(per_group):

            def place(turn, _):
                for part in range(unroll):
                    column = turn * unroll + part
                    index = arrival_words[
                        group_index * per_group + request, seq_index * share_blocks + column
                    ]
                    placed_ref[request * share_blocks + column, plane] = arrived[plane][
                        jnp.clip(index, 0, positions - 1)
                    ]
                return 0

            lax.fori_loop(0, share_blocks // unroll, place, 0)
    for step in steps:
        part_copy(step).wait_send()
        stat_copy(step).wait_send()
        att_copy(step).wait_send()
    own_blocks(planes - 1).wait()
    for step in near_steps:
        block_copy(planes - 1, step).wait_recv()
    for plane in range(planes):
        for step in far_steps:
            far_copy(plane, step).wait_send()
    for plane in range(planes):
        for step in near_steps:
            if step // group_count != 1:
                block_copy(plane, step).wait_send()
    if far_steps:
        pl.when(hands_over)(tail_handed.wait_send)
        pl.when(relays)(tail_passed.wait_send)
        pl.when(jnp.logical_not(hands_over))(tail_direct.wait_send)
    for step in far_steps:
        far_copy(planes - 1, step).wait_recv()
    if far_steps:
        tail_direct.wait_recv()


def copy_out_kernel(
    placed_in,
    last_in,
    arrival_in,
    scale_in,
    output_in,
    cache_ref,
    scale_ref,
    output_ref,
    arrival_words,
    sems,
    block_sem,
):
    positions, first = placed_in.shape[:2]
    per_group, _, share_blocks = scale_in.shape
    group_index, seq_index = lax.axis_index("grp"), lax.axis_index("seq")
    words = pltpu.make_async_copy(arrival_in, arrival_words, sems.at[0])
    words.start()
    chunks = 8
    share = positions // chunks
    copies = [
        pltpu.make_async_copy(
            placed_in.at[pl.ds(part * share, share)],
            cache_ref.at[pl.ds(part * share, share), pl.ds(0, first)],
            sems.at[3 + part],
        )
        for part in range(chunks)
    ]
    copies.append(pltpu.make_async_copy(scale_in, scale_ref, sems.at[1]))
    copies.append(pltpu.make_async_copy(output_in, output_ref, sems.at[2]))
    for copy in copies:
        copy.start()
    words.wait()

    def block(position):
        index = arrival_words[
            group_index * per_group + position // share_blocks,
            seq_index * share_blocks + position % share_blocks,
        ]
        return pltpu.make_async_copy(
            last_in.at[jnp.clip(index, 0, positions - 1)],
            cache_ref.at[position, first],
            block_sem,
        )

    def start(position, _):
        block(position).start()
        return 0

    lax.fori_loop(0, positions, start, 0, unroll=4)
    for copy in copies:
        copy.wait()
    pltpu.make_async_copy(last_in, cache_ref.at[:, first], block_sem).wait()


def per_device(queries, cache_pool, block_scale, block_table, lengths, output_weight):
    seq_count = lax.axis_size("seq")
    group_count = lax.axis_size("grp")
    tp_count = lax.axis_size("tp")
    sources = seq_count * group_count
    pool_slots, key_heads, _, block_size, head_size = cache_pool.shape
    batch_rows, table_width = block_table.shape
    per_group = batch_rows // group_count
    share_blocks = table_width // seq_count
    capacity = pool_slots // sources
    heads_here = queries.shape[1]
    groups = heads_here // key_heads
    planes = key_heads * 2
    positions = per_group * share_blocks
    columns = output_weight.shape[1]
    root_scale = 1.0 / math.sqrt(head_size)

    row_share = batch_rows * key_heads * groups // sources
    query_rows = per_group * groups
    f32, bf16 = jnp.float32, jnp.bfloat16
    dma = pltpu.SemaphoreType.DMA
    vmem = pl.BlockSpec(memory_space=pltpu.VMEM)
    hbm = pl.BlockSpec(memory_space=pltpu.HBM)
    here = batch_rows // tp_count
    results = pl.pallas_call(
        functools.partial(
            exchange_kernel, (seq_count, group_count, tp_count, per_group, root_scale)
        ),
        out_shape=(
            pltpu.VMEM((positions, planes - 1, block_size, head_size), bf16),
            pltpu.VMEM((positions, block_size, head_size), bf16),
            pltpu.VMEM((batch_rows, table_width), jnp.int32),
            pltpu.VMEM((per_group, planes, share_blocks), bf16),
            pltpu.VMEM((here, columns), bf16),
        ),
        in_specs=[hbm, hbm, hbm, hbm, hbm, hbm],
        out_specs=(vmem,) * 5,
        scratch_shapes=[
            pltpu.SMEM((batch_rows,), jnp.int32),
            pltpu.VMEM((batch_rows, table_width), jnp.int32),
            pltpu.VMEM((planes, pool_slots), bf16),
            pltpu.VMEM((key_heads, query_rows, head_size), bf16),
            [pltpu.VMEM((pool_slots, block_size, head_size), bf16) for _ in range(planes)],
            pltpu.VMEM((planes, sources, capacity, block_size, head_size), bf16),
            [pltpu.VMEM((pool_slots, block_size, head_size), bf16) for _ in range(planes - 1)],
            pltpu.VMEM((heads_here * head_size, columns), bf16),
            pltpu.VMEM((group_count, key_heads, query_rows, head_size), bf16),
            pltpu.VMEM((sources, query_rows, capacity * block_size), f32),
            pltpu.VMEM((group_count, query_rows, block_size), f32),
            pltpu.VMEM((group_count, query_rows, block_size), f32),
            pltpu.VMEM((group_count, query_rows, head_size), f32),
            pltpu.VMEM((sources, row_share, head_size), f32),
            pltpu.VMEM((sources, row_share, head_size), f32),
            pltpu.VMEM((sources, 1, head_size), f32),
            pltpu.VMEM((sources, 1, head_size), f32),
            pltpu.VMEM((sources, row_share, head_size), bf16),
            pltpu.VMEM((tp_count, here, columns), f32),
            pltpu.VMEM((tp_count, here, columns), f32),
            pltpu.VMEM((sources, planes, pool_slots), bf16),
            pltpu.VMEM((planes, pool_slots), f32),
            pltpu.VMEM((capacity, batch_rows, table_width), jnp.int32),
            pltpu.SMEM((planes, pool_slots), f32),
            pltpu.SMEM((batch_rows, table_width), jnp.int32),
            pltpu.SMEM((capacity, batch_rows, table_width), jnp.int32),
            pltpu.VMEM((capacity, table_width), jnp.int32),
            pltpu.SMEM((capacity, table_width), jnp.int32),
            dma((planes + 1,)),
            dma((planes + 3,)),
            dma((7 + key_heads * per_group,)),
            dma((planes, sources)),
            dma((planes, sources)),
            pltpu.VMEM((max(capacity // 4, 1), block_size, head_size), bf16),
            dma((5,)),
            dma((group_count,)),
            dma((group_count,)),
            dma((sources,)),
            dma((sources,)),
            dma((sources,)),
            dma((sources,)),
            dma((sources,)),
            dma((sources,)),
            pltpu.SemaphoreType.REGULAR((tp_count,)),
            pltpu.SemaphoreType.REGULAR((tp_count,)),
            dma((sources,)),
            dma((sources,)),
            dma((tp_count,)),
            dma((tp_count,)),
        ],
        compiler_params=pltpu.CompilerParams(
            collective_id=0, has_side_effects=True, vmem_limit_bytes=40 * 2**20
        ),
    )(
        *(
            pltpu.with_memory_space_constraint(operand, pltpu.HBM)
            for operand in (
                lengths,
                block_table,
                block_scale.reshape(pool_slots, planes).T,
                queries,
                cache_pool.reshape(pool_slots, planes, block_size, head_size),
                output_weight,
            )
        )
    )
    decode_cache, decode_scale, output = pl.pallas_call(
        copy_out_kernel,
        out_shape=(
            jax.ShapeDtypeStruct((positions, planes, block_size, head_size), bf16),
            jax.ShapeDtypeStruct(results[3].shape, bf16),
            jax.ShapeDtypeStruct(results[4].shape, bf16),
        ),
        in_specs=[vmem] * 5,
        out_specs=(hbm,) * 3,
        scratch_shapes=[
            pltpu.SMEM((batch_rows, table_width), jnp.int32),
            dma((11,)),
            dma,
        ],
        compiler_params=pltpu.CompilerParams(vmem_limit_bytes=16 * 2**20),
    )(*(pltpu.with_memory_space_constraint(r, pltpu.VMEM) for r in results))
    return (
        output,
        decode_cache.reshape(per_group, share_blocks, key_heads, 2, block_size, head_size),
        decode_scale.transpose(0, 2, 1).reshape(per_group, share_blocks, key_heads, 2),
    )


def solution(mesh):
    placed = (
        P("grp", "tp", None),
        P(("seq", "grp"), "tp", None, None, None),
        P(("seq", "grp"), "tp", None),
        P(),
        P(),
        P("tp", ("seq", "grp")),
    )
    return jax.shard_map(
        per_device,
        mesh=mesh,
        in_specs=placed,
        out_specs=(
            P("tp", ("seq", "grp")),
            P("grp", "seq", "tp", None, None, None),
            P("grp", "seq", "tp", None),
        ),
        check_vma=False,
    )
```

```python
import functools
import math

import jax
import jax.numpy as jnp
from jax import lax
from jax.experimental import pallas as pl
from jax.experimental.pallas import tpu as pltpu
from jax.sharding import PartitionSpec as P

MESH = pl.DeviceIdType.MESH
absent_score = -1e30
absent_limit = -1e29


def xor_index(index, mask):
    out = index
    bit = 1
    while bit <= mask:
        if mask & bit:
            out = out + bit - 2 * bit * ((index // bit) % 2)
        bit *= 2
    return out


def exchange_kernel(
    dims,
    lengths_in,
    table_in,
    block_scale_in,
    queries_in,
    pool_ref,
    weight_ref,
    placed_ref,
    last_ref,
    arrival_rows,
    scales_out_ref,
    output_ref,
    lengths_ref,
    table_ref,
    block_scale_ref,
    queries_ref,
    raw,
    send,
    arrived,
    weights,
    all_queries,
    scores,
    peaks,
    sums,
    accums,
    parts,
    parts_in,
    stats,
    stats_in,
    attended,
    projected,
    projected_in,
    scales_in,
    scales_wide,
    pick_rows,
    scale_words,
    arrival_words,
    pick_words,
    slot_rows,
    slot_words,
    load_sems,
    local_sems,
    word_sems,
    block_send,
    block_recv,
    tail_blocks,
    tail_sems,
    query_send,
    query_recv,
    scale_send,
    scale_recv,
    part_send,
    part_recv,
    stat_send,
    stat_recv,
    known_below,
    known_above,
    att_send,
    att_recv,
    proj_send,
    proj_recv,
):
    seq_count, group_count, tp_count, per_group, root_scale = dims
    sources = seq_count * group_count
    seq_index = lax.axis_index("seq")
    group_index = lax.axis_index("grp")
    tp_index = lax.axis_index("tp")
    me = seq_index * group_count + group_index
    planes, _, capacity, block_size, head_size = send.shape
    arrived = [*arrived, last_ref]
    pool_slots = raw[0].shape[0]
    key_heads = planes // 2
    query_rows = all_queries.shape[2]
    groups = query_rows // per_group
    batch_rows, table_width = table_ref.shape
    share_blocks = table_width // seq_count
    positions = per_group * share_blocks
    row_share = parts.shape[1]
    per_tile = groups // row_share
    f32, bf16 = jnp.float32, jnp.bfloat16

    def pool_load(plane):
        return pltpu.make_async_copy(pool_ref.at[:, plane], raw[plane], load_sems.at[plane])

    table_load = pltpu.make_async_copy(table_in, table_ref, word_sems.at[4])
    small_loads = [
        pltpu.make_async_copy(lengths_in, lengths_ref, word_sems.at[5]),
        pltpu.make_async_copy(block_scale_in, block_scale_ref, word_sems.at[6]),
    ] + [
        pltpu.make_async_copy(
            queries_in.at[request, pl.ds(head * groups, groups)],
            queries_ref.at[head, pl.ds(request * groups, groups)],
            word_sems.at[7 + head * per_group + request],
        )
        for head in range(key_heads)
        for request in range(per_group)
    ]
    table_load.start()
    pool_load(0).start()

    def source_device(other):
        return {"seq": other // group_count, "grp": other % group_count}

    barrier = pltpu.get_barrier_semaphore()
    for step in reversed(range(1, sources)):
        pl.semaphore_signal(
            barrier, inc=1, device_id=source_device(xor_index(me, step)), device_id_type=MESH
        )
    below, above = tp_index > 0, tp_index < tp_count - 1

    @pl.when(above)
    def _():
        pl.semaphore_signal(
            barrier, inc=1, device_id={"tp": tp_index + 1}, device_id_type=MESH
        )

    wide = (batch_rows, table_width)
    table_load.wait()
    table = table_ref[...]
    row_of = lax.broadcasted_iota(jnp.int32, wide, 0)
    col_of = lax.broadcasted_iota(jnp.int32, wide, 1)
    square = (table_width, table_width)
    upper = lax.broadcasted_iota(jnp.int32, square, 0)
    lower = lax.broadcasted_iota(jnp.int32, square, 1)
    alike = upper // share_blocks == lower // share_blocks
    all_alike = jnp.where(alike, 1.0, 0.0).astype(bf16)
    earlier = jnp.where(alike, jnp.where(upper < lower, 1.0, 0.0), 0.0).astype(bf16)
    owner = table // pool_slots
    local = (table % pool_slots).astype(f32)

    def ranks(theirs):
        ones = jnp.where(theirs, 1.0, 0.0).astype(bf16)
        rank = jnp.dot(ones, earlier, preferred_element_type=f32)
        whole = jnp.dot(ones, all_alike, preferred_element_type=f32)
        for request in range(batch_rows):
            last = request // per_group * per_group + per_group
            for later in range(request + 1, last):
                rank = rank + jnp.where(row_of == later, whole[request : request + 1], 0.0)
        return rank

    range_of = jnp.where(upper // share_blocks == lower, 1.0, 0.0).astype(bf16)
    own_rank = jnp.where(owner == me, ranks(owner == me), -1.0)

    rank_rows = lax.broadcasted_iota(jnp.int32, (capacity, table_width), 0).astype(f32)
    slots = jnp.zeros((capacity, table_width), f32)
    for request in range(batch_rows):
        column = upper // share_blocks + request // per_group * seq_count
        slots += jnp.dot(
            jnp.where(
                own_rank[request : request + 1] == rank_rows, local[request : request + 1], 0.0
            ).astype(bf16),
            jnp.where(column == lower, 1.0, 0.0).astype(bf16),
            preferred_element_type=f32,
        )
    slot_rows[...] = slots.astype(jnp.int32)
    slot_copy = pltpu.make_async_copy(slot_rows, slot_words, word_sems.at[0])
    slot_copy.start()

    def pick(values):
        for within in range(capacity):
            pick_rows[within] = jnp.dot(
                jnp.where(own_rank == within, values, 0.0).astype(bf16),
                range_of,
                preferred_element_type=f32,
            ).astype(jnp.int32)
        return pltpu.make_async_copy(pick_rows, pick_words, word_sems.at[1])

    own_queries = pltpu.make_async_copy(queries_ref, all_queries.at[group_index], local_sems.at[0])
    pl.semaphore_wait(barrier, sources - 1 + jnp.where(below, 1, 0))

    def query_copy(step):
        return pltpu.make_async_remote_copy(
            src_ref=queries_ref,
            dst_ref=all_queries.at[group_index],
            send_sem=query_send.at[step],
            recv_sem=query_recv.at[step],
            device_id={"grp": xor_index(group_index, step)},
            device_id_type=MESH,
        )

    def scale_copy(step):
        return pltpu.make_async_remote_copy(
            src_ref=block_scale_ref,
            dst_ref=scales_in.at[me],
            send_sem=scale_send.at[step],
            recv_sem=scale_recv.at[step],
            device_id=source_device(xor_index(me, step)),
            device_id_type=MESH,
        )

    own_scales = pltpu.make_async_copy(block_scale_ref, scales_in.at[me], local_sems.at[1])

    def block_copy(plane, step):
        other = xor_index(me, step)
        return pltpu.make_async_remote_copy(
            src_ref=send.at[plane, other],
            dst_ref=arrived[plane].at[pl.ds(me * capacity, capacity)],
            send_sem=block_send.at[plane, step],
            recv_sem=block_recv.at[plane, step],
            device_id=source_device(other),
            device_id_type=MESH,
        )

    def own_blocks(plane):
        return pltpu.make_async_copy(
            send.at[plane, me],
            arrived[plane].at[pl.ds(me * capacity, capacity)],
            local_sems.at[2 + plane],
        )

    steps = sorted(range(1, sources), key=lambda s: (s // group_count == 0, s % group_count, s))
    near_steps = [s for s in steps if (s // group_count).bit_count() <= 1]
    far_steps = [s for s in steps if s not in near_steps]

    tail_plane, tail_step = planes - 1, far_steps[-1] if far_steps else 0
    kept = capacity - tail_blocks.shape[0]
    origin = (seq_count - 1) * group_count
    to_relay = group_count * (1 << max(tail_step // group_count, 1).bit_length() - 1)
    to_relay += tail_step % group_count
    hands_over = seq_index == seq_count - 1
    relays = seq_index == (seq_count - 1) ^ (to_relay // group_count)

    def far_copy(plane, step):
        if (plane, step) != (tail_plane, tail_step):
            return block_copy(plane, step)
        other = xor_index(me, step)
        return pltpu.make_async_remote_copy(
            src_ref=send.at[plane, other, pl.ds(0, kept)],
            dst_ref=arrived[plane].at[pl.ds(me * capacity, kept)],
            send_sem=block_send.at[plane, step],
            recv_sem=block_recv.at[plane, step],
            device_id=source_device(other),
            device_id_type=MESH,
        )

    def tail_copy(source, owner, route, sent, received):
        return pltpu.make_async_remote_copy(
            src_ref=source,
            dst_ref=arrived[tail_plane].at[
                pl.ds(owner * capacity + kept, capacity - kept)
            ],
            send_sem=sent,
            recv_sem=received,
            device_id=source_device(xor_index(me, route)),
            device_id_type=MESH,
        )

    if far_steps:
        tail_source = send.at[tail_plane, xor_index(me, tail_step), pl.ds(kept, capacity - kept)]
        tail_direct = tail_copy(
            tail_source, me, tail_step, tail_sems.at[0], tail_sems.at[1]
        )
        tail_passed = tail_copy(
            tail_blocks,
            xor_index(me, to_relay),
            tail_step ^ to_relay,
            tail_sems.at[2],
            tail_sems.at[1],
        )
        tail_handed = pltpu.make_async_remote_copy(
            src_ref=tail_source,
            dst_ref=tail_blocks,
            send_sem=tail_sems.at[3],
            recv_sem=tail_sems.at[4],
            device_id=source_device(xor_index(me, to_relay)),
            device_id_type=MESH,
        )

    def picked(other, within, request):
        group = other % group_count
        return pick_words[within, group * per_group + request, other // group_count]

    def slot_of(other, within):
        slot = slot_words[within, other % group_count * seq_count + other // group_count]
        return jnp.clip(slot, 0, pool_slots - 1)

    def sort_blocks(plane, other):
        def place(within, _):
            send[plane, other, within] = raw[plane][slot_of(other, within)]
            return 0

        lax.fori_loop(0, capacity, place, 0)

    def sort_plane(plane):
        def place(other, _):
            sort_blocks(plane, other)
            return 0

        lax.fori_loop(0, sources, place, 0)

    def send_plane(plane, chosen):
        for step in chosen:
            block_copy(plane, step).start()

    slot_copy.wait()
    pool_load(0).wait()
    for place, step in enumerate(near_steps):
        other = xor_index(me, step)
        for within in range(capacity):
            send[0, other, within] = raw[0][slot_of(other, within)]
        if place:
            block_copy(0, near_steps[place - 1]).start()
    sort_blocks(0, me)
    block_copy(0, near_steps[-1]).start()
    for copy in small_loads:
        copy.start()
    for plane in range(1, planes):
        pool_load(plane).start()
    for copy in small_loads:
        copy.wait()
    own_queries.start()
    for step in range(1, group_count):
        query_copy(step).start()
    for step in steps:
        scale_copy(step).start()
    own_scales.start()
    weight_load = pltpu.make_async_copy(weight_ref, weights, load_sems.at[planes])
    weight_load.start()
    for step in far_steps:
        sort_blocks(0, xor_index(me, step))
    for plane in range(1, planes):
        pool_load(plane).wait()
        sort_plane(plane)
        if plane == 1:
            send_plane(plane, near_steps)
    if far_steps:
        pl.when(hands_over)(tail_handed.start)
    for plane in range(planes):
        own_blocks(plane).start()

    arrival = jnp.zeros(wide, f32)
    for source in range(sources):
        theirs = owner == source
        arrival = jnp.where(theirs, ranks(theirs) + source * capacity, arrival)
    arrival_rows[...] = arrival.astype(jnp.int32)
    context = jnp.full(wide, lengths_ref[0], jnp.int32)
    for request in range(1, batch_rows):
        context = jnp.where(row_of == request, lengths_ref[request], context)
    live = jnp.clip(context - col_of * block_size, 0, block_size).astype(f32)
    scales_wide[...] = block_scale_ref[...].astype(f32)
    word_copies = [
        pick(live),
        pltpu.make_async_copy(arrival_rows, arrival_words, word_sems.at[2]),
        pltpu.make_async_copy(scales_wide, scale_words, word_sems.at[3]),
    ]
    for copy in word_copies:
        copy.start()
    for copy in word_copies:
        copy.wait()

    own_queries.wait()
    for step in range(1, group_count):
        query_copy(step).wait()

    lanes = lax.broadcasted_iota(jnp.int32, (query_rows, block_size), 1)
    row_ids = lax.broadcasted_iota(jnp.int32, (query_rows, block_size), 0)
    share_lanes = lax.broadcasted_iota(jnp.int32, (row_share, head_size), 1)
    share_rows = lax.broadcasted_iota(jnp.int32, (row_share, head_size), 0)
    for head in range(key_heads):
        peaks[...] = jnp.full_like(peaks, absent_score)
        sums[...] = jnp.zeros_like(sums)
        accums[...] = jnp.zeros_like(accums)

        def score_blocks(other, _):
            group = other % group_count
            keys = send[2 * head, other].reshape(capacity * block_size, head_size)
            raw_scores = lax.dot_general(
                all_queries[group, head],
                keys,
                (((1,), (1,)), ((), ())),
                preferred_element_type=jnp.float32,
            )
            highest = peaks[group]
            for within in range(capacity):
                limit = jnp.full(lanes.shape, picked(other, within, 0), jnp.int32)
                for request in range(1, per_group):
                    limit = jnp.where(
                        row_ids >= request * groups, picked(other, within, request), limit
                    )
                part = raw_scores[:, within * block_size : (within + 1) * block_size]
                part = part * scale_words[2 * head, slot_of(other, within)] * root_scale
                part = jnp.where(lanes < limit, part, absent_score)
                scores[other, :, within * block_size : (within + 1) * block_size] = part
                highest = jnp.maximum(highest, part)
            peaks[group] = highest
            return 0

        lax.fori_loop(0, sources, score_blocks, 0)
        for group in range(group_count):
            peaks[group] = jnp.broadcast_to(
                jnp.max(peaks[group], axis=1, keepdims=True), lanes.shape
            )

        def weigh_blocks(other, _):
            group = other % group_count
            peak = peaks[group]
            total = sums[group]
            pieces = []
            for within in range(capacity):
                part = scores[other, :, within * block_size : (within + 1) * block_size]
                weight = jnp.where(part > absent_limit, jnp.exp(part - peak), 0.0)
                total = total + weight
                pieces.append(
                    (weight * scale_words[2 * head + 1, slot_of(other, within)]).astype(bf16)
                )
            sums[group] = total
            values = send[2 * head + 1, other].reshape(capacity * block_size, head_size)
            accums[group] += jnp.dot(
                jnp.concatenate(pieces, axis=1), values, preferred_element_type=jnp.float32
            )
            return 0

        lax.fori_loop(0, sources, weigh_blocks, 0)
        for group in range(group_count):
            total = jnp.broadcast_to(jnp.sum(sums[group], axis=1, keepdims=True), lanes.shape)
            for request in range(per_group):
                tile = (group * key_heads + head) * per_group + request
                for piece in range(per_tile):
                    low = request * groups + piece * row_share
                    place = tile * per_tile + piece
                    parts[place] = accums[group, low : low + row_share]
                    stats[place] = jnp.sum(
                        jnp.where(
                            share_lanes == share_rows, peaks[group, low : low + row_share], 0.0
                        )
                        + jnp.where(
                            share_lanes == share_rows + row_share,
                            total[low : low + row_share],
                            0.0,
                        ),
                        axis=0,
                        keepdims=True,
                    )

    def part_copy(step):
        other = xor_index(me, step)
        return pltpu.make_async_remote_copy(
            src_ref=parts.at[other],
            dst_ref=parts_in.at[me],
            send_sem=part_send.at[step],
            recv_sem=part_recv.at[step],
            device_id=source_device(other),
            device_id_type=MESH,
        )

    def stat_copy(step):
        other = xor_index(me, step)
        return pltpu.make_async_remote_copy(
            src_ref=stats.at[other],
            dst_ref=stats_in.at[me],
            send_sem=stat_send.at[step],
            recv_sem=stat_recv.at[step],
            device_id=source_device(other),
            device_id_type=MESH,
        )

    for step in steps:
        stat_copy(step).start()
        part_copy(step).start()
    parts_in[me] = parts[me]
    stats_in[me] = stats[me]
    for plane in range(2, min(planes, 3)):
        send_plane(plane, near_steps)

    @pl.when(below)
    def _():
        pl.semaphore_signal(
            known_above.at[0], inc=1, device_id={"tp": tp_index - 1}, device_id_type=MESH
        )

    @pl.when(above)
    def _():
        pl.semaphore_wait(known_above.at[0], 1)

    for reach in range(1, tp_count - 1):

        @pl.when(jnp.logical_and(tp_index >= reach, above))
        def _():
            pl.semaphore_signal(
                known_below.at[reach], inc=1, device_id={"tp": tp_index + 1}, device_id_type=MESH
            )

        @pl.when(jnp.logical_and(tp_index + reach < tp_count, below))
        def _():
            pl.semaphore_signal(
                known_above.at[reach], inc=1, device_id={"tp": tp_index - 1}, device_id_type=MESH
            )

        @pl.when(tp_index - 1 >= reach)
        def _():
            pl.semaphore_wait(known_below.at[reach], 1)

        @pl.when(tp_index + 1 + reach < tp_count)
        def _():
            pl.semaphore_wait(known_above.at[reach], 1)

    for step in steps:
        stat_copy(step).wait_recv()
        part_copy(step).wait_recv()

    def spread(source, first):
        return jnp.broadcast_to(
            jnp.sum(
                jnp.where(
                    share_lanes == share_rows + first,
                    jnp.broadcast_to(stats_in[source], share_lanes.shape),
                    0.0,
                ),
                axis=1,
                keepdims=True,
            ),
            share_lanes.shape,
        )

    source_peaks = [spread(source, 0) for source in range(sources)]
    highest = functools.reduce(jnp.maximum, source_peaks)
    numerator = jnp.zeros_like(highest)
    denominator = jnp.zeros_like(highest)
    for source in range(sources):
        factor = jnp.exp(source_peaks[source] - highest)
        numerator += parts_in[source] * factor
        denominator += spread(source, row_share) * factor
    attended[me] = (numerator / denominator).astype(jnp.bfloat16)

    def att_copy(step):
        return pltpu.make_async_remote_copy(
            src_ref=attended.at[me],
            dst_ref=attended.at[me],
            send_sem=att_send.at[step],
            recv_sem=att_recv.at[step],
            device_id=source_device(xor_index(me, step)),
            device_id_type=MESH,
        )

    weight_load.wait()
    for step in steps:
        att_copy(step).start()
    for plane in range(3, planes):
        send_plane(plane, near_steps)
    for step in steps:
        att_copy(step).wait_recv()
    for plane in range(planes):
        for step in near_steps:
            if step // group_count == 1:
                block_copy(plane, step).wait_send()
    if far_steps:

        @pl.when(relays)
        def _():
            tail_handed.wait_recv()
            tail_passed.start()

    for plane in range(planes):
        for step in far_steps:
            far_copy(plane, step).start()
    if far_steps:
        pl.when(jnp.logical_not(hands_over))(tail_direct.start)

    rows = sources * row_share
    gathered = attended[...].astype(f32).reshape(rows, head_size)
    row = lax.broadcasted_iota(jnp.int32, (rows, head_size), 0)
    row_head = (row // (groups * per_group)) % key_heads * groups + row % groups
    left = jnp.concatenate(
        [
            jnp.where(row_head == head, gathered, 0.0).astype(jnp.bfloat16)
            for head in range(key_heads * groups)
        ],
        axis=1,
    )
    columns = weights.shape[1]
    width = min(columns, 256)
    here = batch_rows // tp_count
    for low in range(0, columns, width):
        product = jnp.dot(left, weights[:, low : low + width], preferred_element_type=jnp.float32)
        for request in range(batch_rows):
            group, inner = request // per_group, request % per_group
            total = jnp.zeros((1, width), jnp.float32)
            for head in range(key_heads):
                tile = (group * key_heads + head) * per_group + inner
                total += jnp.sum(
                    product[tile * groups : (tile + 1) * groups], axis=0, keepdims=True
                )
            projected[request // here, pl.ds(request % here, 1), low : low + width] = total

    def proj_copy(step):
        other = xor_index(tp_index, step)
        return pltpu.make_async_remote_copy(
            src_ref=projected.at[other],
            dst_ref=projected_in.at[tp_index],
            send_sem=proj_send.at[step],
            recv_sem=proj_recv.at[step],
            device_id={"tp": other},
            device_id_type=MESH,
        )

    for step in range(1, tp_count):
        proj_copy(step).start()
    projected_in[tp_index] = projected[tp_index]
    for step in range(1, tp_count):
        proj_copy(step).wait()
    total = projected_in[0]
    for source in range(1, tp_count):
        total += projected_in[source]
    output_ref[...] = total.astype(output_ref.dtype)

    own_scales.wait()
    for step in steps:
        scale_copy(step).wait()
    slot_ids = lax.broadcasted_iota(jnp.int32, (pool_slots, table_width), 0)
    wanted = jnp.where(
        lax.broadcasted_iota(jnp.int32, (table_width, share_blocks), 0)
        == lax.broadcasted_iota(jnp.int32, (table_width, share_blocks), 1)
        + seq_index * share_blocks,
        1.0,
        0.0,
    ).astype(bf16)
    for request in range(per_group):
        slots = table_ref[pl.ds(group_index * per_group + request, 1), :]
        found = jnp.zeros((planes, table_width), f32)
        for source in range(sources):
            onehot = jnp.where(slots == slot_ids + source * pool_slots, 1.0, 0.0).astype(bf16)
            found += jnp.dot(scales_in[source], onehot, preferred_element_type=f32)
        scales_out_ref[request] = jnp.dot(
            found.astype(bf16), wanted, preferred_element_type=f32
        ).astype(bf16)

    unroll = 4 if share_blocks % 4 == 0 else 1
    for plane in range(planes - 1):
        own_blocks(plane).wait()
        for step in steps:
            (block_copy if step in near_steps else far_copy)(plane, step).wait_recv()
        for request in range(per_group):

            def place(turn, _):
                for part in range(unroll):
                    column = turn * unroll + part
                    index = arrival_words[
                        group_index * per_group + request, seq_index * share_blocks + column
                    ]
                    placed_ref[request * share_blocks + column, plane] = arrived[plane][
                        jnp.clip(index, 0, positions - 1)
                    ]
                return 0

            lax.fori_loop(0, share_blocks // unroll, place, 0)
    for step in steps:
        part_copy(step).wait_send()
        stat_copy(step).wait_send()
        att_copy(step).wait_send()
    own_blocks(planes - 1).wait()
    for step in near_steps:
        block_copy(planes - 1, step).wait_recv()
    for plane in range(planes):
        for step in far_steps:
            far_copy(plane, step).wait_send()
    for plane in range(planes):
        for step in near_steps:
            if step // group_count != 1:
                block_copy(plane, step).wait_send()
    if far_steps:
        pl.when(hands_over)(tail_handed.wait_send)
        pl.when(relays)(tail_passed.wait_send)
        pl.when(jnp.logical_not(hands_over))(tail_direct.wait_send)
    for step in far_steps:
        far_copy(planes - 1, step).wait_recv()
    if far_steps:
        tail_direct.wait_recv()


def copy_out_kernel(
    placed_in,
    last_in,
    arrival_in,
    scale_in,
    output_in,
    cache_ref,
    scale_ref,
    output_ref,
    arrival_words,
    sems,
    block_sem,
):
    positions, first = placed_in.shape[:2]
    per_group, _, share_blocks = scale_in.shape
    group_index, seq_index = lax.axis_index("grp"), lax.axis_index("seq")
    words = pltpu.make_async_copy(arrival_in, arrival_words, sems.at[0])
    words.start()
    chunks = 8
    share = positions // chunks
    copies = [
        pltpu.make_async_copy(
            placed_in.at[pl.ds(part * share, share)],
            cache_ref.at[pl.ds(part * share, share), pl.ds(0, first)],
            sems.at[3 + part],
        )
        for part in range(chunks)
    ]
    copies.append(pltpu.make_async_copy(scale_in, scale_ref, sems.at[1]))
    copies.append(pltpu.make_async_copy(output_in, output_ref, sems.at[2]))
    for copy in copies:
        copy.start()
    words.wait()

    def block(position):
        index = arrival_words[
            group_index * per_group + position // share_blocks,
            seq_index * share_blocks + position % share_blocks,
        ]
        return pltpu.make_async_copy(
            last_in.at[jnp.clip(index, 0, positions - 1)],
            cache_ref.at[position, first],
            block_sem,
        )

    def start(position, _):
        block(position).start()
        return 0

    lax.fori_loop(0, positions, start, 0, unroll=4)
    for copy in copies:
        copy.wait()
    pltpu.make_async_copy(last_in, cache_ref.at[:, first], block_sem).wait()


def per_device(queries, cache_pool, block_scale, block_table, lengths, output_weight):
    seq_count = lax.axis_size("seq")
    group_count = lax.axis_size("grp")
    tp_count = lax.axis_size("tp")
    sources = seq_count * group_count
    pool_slots, key_heads, _, block_size, head_size = cache_pool.shape
    batch_rows, table_width = block_table.shape
    per_group = batch_rows // group_count
    share_blocks = table_width // seq_count
    capacity = pool_slots // sources
    heads_here = queries.shape[1]
    groups = heads_here // key_heads
    planes = key_heads * 2
    positions = per_group * share_blocks
    columns = output_weight.shape[1]
    root_scale = 1.0 / math.sqrt(head_size)

    row_share = batch_rows * key_heads * groups // sources
    query_rows = per_group * groups
    f32, bf16 = jnp.float32, jnp.bfloat16
    dma = pltpu.SemaphoreType.DMA
    vmem = pl.BlockSpec(memory_space=pltpu.VMEM)
    hbm = pl.BlockSpec(memory_space=pltpu.HBM)
    here = batch_rows // tp_count
    results = pl.pallas_call(
        functools.partial(
            exchange_kernel, (seq_count, group_count, tp_count, per_group, root_scale)
        ),
        out_shape=(
            pltpu.VMEM((positions, planes - 1, block_size, head_size), bf16),
            pltpu.VMEM((positions, block_size, head_size), bf16),
            pltpu.VMEM((batch_rows, table_width), jnp.int32),
            pltpu.VMEM((per_group, planes, share_blocks), bf16),
            pltpu.VMEM((here, columns), bf16),
        ),
        in_specs=[hbm, hbm, hbm, hbm, hbm, hbm],
        out_specs=(vmem,) * 5,
        scratch_shapes=[
            pltpu.SMEM((batch_rows,), jnp.int32),
            pltpu.VMEM((batch_rows, table_width), jnp.int32),
            pltpu.VMEM((planes, pool_slots), bf16),
            pltpu.VMEM((key_heads, query_rows, head_size), bf16),
            [pltpu.VMEM((pool_slots, block_size, head_size), bf16) for _ in range(planes)],
            pltpu.VMEM((planes, sources, capacity, block_size, head_size), bf16),
            [pltpu.VMEM((pool_slots, block_size, head_size), bf16) for _ in range(planes - 1)],
            pltpu.VMEM((heads_here * head_size, columns), bf16),
            pltpu.VMEM((group_count, key_heads, query_rows, head_size), bf16),
            pltpu.VMEM((sources, query_rows, capacity * block_size), f32),
            pltpu.VMEM((group_count, query_rows, block_size), f32),
            pltpu.VMEM((group_count, query_rows, block_size), f32),
            pltpu.VMEM((group_count, query_rows, head_size), f32),
            pltpu.VMEM((sources, row_share, head_size), f32),
            pltpu.VMEM((sources, row_share, head_size), f32),
            pltpu.VMEM((sources, 1, head_size), f32),
            pltpu.VMEM((sources, 1, head_size), f32),
            pltpu.VMEM((sources, row_share, head_size), bf16),
            pltpu.VMEM((tp_count, here, columns), f32),
            pltpu.VMEM((tp_count, here, columns), f32),
            pltpu.VMEM((sources, planes, pool_slots), bf16),
            pltpu.VMEM((planes, pool_slots), f32),
            pltpu.VMEM((capacity, batch_rows, table_width), jnp.int32),
            pltpu.SMEM((planes, pool_slots), f32),
            pltpu.SMEM((batch_rows, table_width), jnp.int32),
            pltpu.SMEM((capacity, batch_rows, table_width), jnp.int32),
            pltpu.VMEM((capacity, table_width), jnp.int32),
            pltpu.SMEM((capacity, table_width), jnp.int32),
            dma((planes + 1,)),
            dma((planes + 3,)),
            dma((7 + key_heads * per_group,)),
            dma((planes, sources)),
            dma((planes, sources)),
            pltpu.VMEM((max(capacity // 8, 1), block_size, head_size), bf16),
            dma((5,)),
            dma((group_count,)),
            dma((group_count,)),
            dma((sources,)),
            dma((sources,)),
            dma((sources,)),
            dma((sources,)),
            dma((sources,)),
            dma((sources,)),
            pltpu.SemaphoreType.REGULAR((tp_count,)),
            pltpu.SemaphoreType.REGULAR((tp_count,)),
            dma((sources,)),
            dma((sources,)),
            dma((tp_count,)),
            dma((tp_count,)),
        ],
        compiler_params=pltpu.CompilerParams(
            collective_id=0, has_side_effects=True, vmem_limit_bytes=40 * 2**20
        ),
    )(
        *(
            pltpu.with_memory_space_constraint(operand, pltpu.HBM)
            for operand in (
                lengths,
                block_table,
                block_scale.reshape(pool_slots, planes).T,
                queries,
                cache_pool.reshape(pool_slots, planes, block_size, head_size),
                output_weight,
            )
        )
    )
    decode_cache, decode_scale, output = pl.pallas_call(
        copy_out_kernel,
        out_shape=(
            jax.ShapeDtypeStruct((positions, planes, block_size, head_size), bf16),
            jax.ShapeDtypeStruct(results[3].shape, bf16),
            jax.ShapeDtypeStruct(results[4].shape, bf16),
        ),
        in_specs=[vmem] * 5,
        out_specs=(hbm,) * 3,
        scratch_shapes=[
            pltpu.SMEM((batch_rows, table_width), jnp.int32),
            dma((11,)),
            dma,
        ],
        compiler_params=pltpu.CompilerParams(vmem_limit_bytes=16 * 2**20),
    )(*(pltpu.with_memory_space_constraint(r, pltpu.VMEM) for r in results))
    return (
        output,
        decode_cache.reshape(per_group, share_blocks, key_heads, 2, block_size, head_size),
        decode_scale.transpose(0, 2, 1).reshape(per_group, share_blocks, key_heads, 2),
    )


def solution(mesh):
    placed = (
        P("grp", "tp", None),
        P(("seq", "grp"), "tp", None, None, None),
        P(("seq", "grp"), "tp", None),
        P(),
        P(),
        P("tp", ("seq", "grp")),
    )
    return jax.shard_map(
        per_device,
        mesh=mesh,
        in_specs=placed,
        out_specs=(
            P("tp", ("seq", "grp")),
            P("grp", "seq", "tp", None, None, None),
            P("grp", "seq", "tp", None),
        ),
        check_vma=False,
    )
```
